128 devices in a mesh: wide: 16 (over x_lo, z, core), narrow: 8 (over x_hi, y).
Axes of the slice: x: 4 (x_hi: 2, x_lo: 2; x = x_hi * 2 + x_lo), y: 4, z: 4, core: 2. Of those that a mesh axis runs over, the one named last changes fastest.
Arguments:
- pixel_stack: float32 [128, 128, 4096], P(('wide', 'narrow')), may hold values from -6 to 6
- quality_weight: float32 [128, 128, 4096], P(('wide', 'narrow')), may hold values from 0.2 to 1
Outputs:
- slope: float32 [128, 4096], P('wide', 'narrow')
- level: float32 [128, 4096], P('wide', 'narrow')
- anomaly: bfloat16 [128, 128, 4096], P(None, 'wide', 'narrow')
The draws below stay inside these ranges and needn't reach their ends.
All inputs are finite; a program needn't handle non-finite values.
Results may differ from the reference program's by a relative error of at most 0.001.
Values sent between devices are 32-bit elements; how exact they have to be, the bound alone decides.
A program may use at most 64 MiB of HBM per device.

```python
import jax
import jax.numpy as jnp
from jax import lax

TSTEPS = 128
ROWS_DEV = 8
H = 128
W = 4096


def steps_of(own_key, dims, shards, low, largest):
    def one(position, parts):
        heights = jax.random.uniform(jax.random.fold_in(jax.random.fold_in(own_key, 6), position), (parts,), jnp.float32, low / len(shards), largest / len(shards))
        return jnp.repeat(jnp.exp(heights), dims[position] // parts).reshape((-1,) + (1,) * (len(dims) - position - 1))

    loudness = one(*shards[0])
    for cut in shards[1:]:
        loudness = loudness * one(*cut)
    return loudness


def noise(key, extent, deviation, most, cuts=(), dtype=jnp.bfloat16):
    result = deviation * jax.random.normal(key, extent, jnp.float32)
    if cuts:
        result = result * steps_of(key, extent, cuts, -0.22, 0.18)
    return jnp.clip(result, -most, most).astype(dtype)


def setup_inputs(seed: int = 0) -> dict:
    key_of = jax.random.split(jax.random.key(seed), 3)
    pixel_stack = noise(key_of[0], (TSTEPS, H, W), 1.0, 6.0, ((0, 128),), jnp.float32)
    quality_weight = jnp.clip(0.2 + 0.8 * jax.random.uniform(key_of[1], (TSTEPS, H, W), jnp.float32) ** steps_of(key_of[1], (TSTEPS, H, W), ((0, 128),), -0.2, 0.2), 0.2, 1.0)
    return {"pixel_stack": pixel_stack, "quality_weight": quality_weight}


def fit_trend(series, weight_series):
    count = series.shape[0]
    centred = ((jnp.arange(count).astype(jnp.float32) - (count - 1) / 2.0) / count).reshape(count, 1, 1)
    weighted = weight_series * series
    first = jnp.sum(weight_series, axis=0)
    second = jnp.sum(weight_series * centred, axis=0)
    third = jnp.sum(weight_series * centred * centred, axis=0)
    plain_sum = jnp.sum(weighted, axis=0)
    moment_sum = jnp.sum(weighted * centred, axis=0)
    determinant = first * third - second * second
    slope = (first * moment_sum - second * plain_sum) / determinant
    level = (third * plain_sum - second * moment_sum) / determinant
    anomaly = (series - level[None] - slope[None] * centred).astype(jnp.bfloat16)
    return slope, level, anomaly


def reference(pixel_stack, quality_weight):
    blocks = H // ROWS_DEV
    series = pixel_stack.reshape(TSTEPS, blocks, ROWS_DEV, W).transpose(1, 0, 2, 3)
    weights = quality_weight.reshape(TSTEPS, blocks, ROWS_DEV, W).transpose(1, 0, 2, 3)
    slope, level, anomaly = lax.map(lambda pair: fit_trend(pair[0], pair[1]), (series, weights))
    slope = slope.reshape(H, W)
    level = level.reshape(H, W)
    anomaly = anomaly.transpose(1, 0, 2, 3).reshape(TSTEPS, H, W)
    return slope, level, anomaly
```

```python
import jax
import jax.numpy as jnp
from jax import lax
from jax.experimental import pallas as pl
from jax.experimental.pallas import tpu as pltpu
from jax.sharding import PartitionSpec as P

MESH = pl.DeviceIdType.MESH
PIECES = 4
LANES = 128
ORDERS = (
    ("xzy", "yzx"),
    ("zyx", "xzy"),
    ("yxz", "zyx"),
    ("xzy", "yxz"),
)
OFFSETS = tuple((u, v) for u in (1, 3, 2, 0) for v in (1, 3, 2, 0) if (u, v) != (0, 0))
OFFSETS = OFFSETS[::4] + OFFSETS[1::4] + OFFSETS[2::4] + OFFSETS[3::4]
VIEWS = {"x": (4, 4), "y": (2, 4, 2), "z": (2, 2, 4)}


def ring(value, shift):
    return lax.rem(value + shift, 4)


def x_parts(x):
    return lax.rem(x, 2), lax.div(x, 2)


def device_of(at, core):
    low, high = x_parts(at["x"])
    return {"wide": low * 8 + at["z"] * 2 + core, "narrow": high * 4 + at["y"]}


def step_of(at, core):
    device = device_of(at, core)
    return device["wide"] * 8 + device["narrow"]


def tile_in_plane(first, at):
    low, high = x_parts(at["x"])
    if first == "x":
        return at["z"] * 4 + at["y"]
    if first == "y":
        return low * 8 + at["z"] * 2 + high
    return low * 8 + high * 4 + at["y"]


def kernel(
    y_ref, w_ref, slope_ref, level_ref, anomaly_ref,
    y_near, w_near, y_all, sums, sums_in, part, part_in, out, fit,
    y_near_sem, w_near_sem, y_all_sem, sums_sem, part_sem, send_sem, out_sem, ready_sem,
):
    wide, narrow = lax.axis_index("wide"), lax.axis_index("narrow")
    core = lax.rem(wide, 2)
    here = {
        "x": lax.div(narrow, 4) * 2 + lax.div(wide, 8),
        "y": lax.rem(narrow, 4),
        "z": lax.rem(lax.div(wide, 2), 4),
    }

    def select(values):
        zero, one = values
        return zero + core * (one - zero)

    def moved(**places):
        return {**here, **places}

    def by_core(function):
        return select([function(c) for c in range(2)])

    def peer_of(piece, shift_second, shift_third):
        places = []
        for c in range(2):
            _, second, third = ORDERS[piece][c]
            at = moved(**{second: ring(here[second], shift_second), third: ring(here[third], shift_third)})
            places.append(device_of(at, c))
        return {axis: select([place[axis] for place in places]) for axis in places[0]}

    def tile_at(piece, u, v):
        def of(c):
            first, second, third = ORDERS[piece][c]
            return tile_in_plane(first, moved(**{second: u, third: v}))

        return by_core(of)

    def place(piece, level):
        return by_core(lambda c: here[ORDERS[piece][c][level]])

    def step_at(piece, slot, u, v):
        def of(c):
            first, second, third = ORDERS[piece][c]
            return step_of(moved(**{first: slot // 2, second: u, third: v}), slot % 2)

        return by_core(of)

    def centred_of(step):
        return (step.astype(jnp.float32) - 63.5) * (1.0 / 128.0)

    barrier = pltpu.get_barrier_semaphore()
    count = 0
    for axis in "xyz":
        for shift in (1, 2, 3):
            for flip in range(2):
                target = device_of(moved(**{axis: ring(here[axis], shift)}), lax.rem(core + flip, 2))
                pl.semaphore_signal(barrier, inc=1, device_id=target, device_id_type=MESH)
                count += 1
    pl.semaphore_signal(barrier, inc=1, device_id=device_of(here, 1 - core), device_id_type=MESH)
    pl.semaphore_wait(barrier, count + 1)

    queues = {"x": [], "y": [], "z": []}
    for piece in range(PIECES):
        for c in range(2):
            first = ORDERS[piece][c][0]
            queues[first] += [(piece, c, shift) for shift in (1, 3, 2, 0)]

    def send_near(piece, c, shift):
        first = ORDERS[piece][c][0]
        where = ring(here[first], shift)
        low, high = x_parts(where)
        slot = here[first] * 2 + core
        for field, near, sem in ((y_ref, y_near, y_near_sem), (w_ref, w_near, w_near_sem)):
            if first == "x":
                source = field.at[low, :, c, high, :, piece]
            elif first == "y":
                source = field.at[:, :, c, :, where, piece]
            else:
                source = field.at[:, where, c, :, :, piece]
            target = near.at[piece, slot].reshape(*VIEWS[first], 8, LANES)

            def remote():
                pltpu.make_async_remote_copy(
                    src_ref=source,
                    dst_ref=target,
                    send_sem=send_sem.at[0],
                    recv_sem=sem.at[piece],
                    device_id=device_of(moved(**{first: where}), c),
                    device_id_type=MESH,
                ).start()

            if shift:
                remote()
            else:

                @pl.when(core == c)
                def _():
                    pltpu.make_async_copy(source, target, sem.at[piece]).start()

                pl.when(core != c)(remote)

    for turn in range(max(len(queue) for queue in queues.values())):
        for axis in "xyz":
            if turn < len(queues[axis]):
                send_near(*queues[axis][turn])

    for axis in "xyz":
        for shift in (1, 2, 3):
            target = device_of(moved(**{axis: ring(here[axis], shift)}), core)
            pl.semaphore_signal(ready_sem, inc=1, device_id=target, device_id_type=MESH)
    pl.semaphore_wait(ready_sem, 9)

    def await_bytes(ref, sem):
        pltpu.make_async_copy(ref, ref, sem).wait()

    def partial_sums(piece):
        own_u, own_v = place(piece, 1), place(piece, 2)
        centred = [centred_of(step_at(piece, slot, own_u, own_v)) for slot in range(8)]

        def one(index, carry):
            u, v = lax.div(index, 4), lax.rem(index, 4)
            tile = tile_at(piece, u, v)
            zero = jnp.zeros((8, LANES), jnp.float32)
            s0, s1, s2, sy, sty = zero, zero, zero, zero, zero
            for slot in range(8):
                w = w_near[piece, slot, tile]
                weighted = w * y_near[piece, slot, tile]
                moment = w * centred[slot]
                s0 += w
                s1 += moment
                s2 += moment * centred[slot]
                sy += weighted
                sty += weighted * centred[slot]
            for i, value in enumerate((s0, s1, s2, sy, sty)):
                sums[piece, u, v, i] = value
            return carry

        lax.fori_loop(0, 16, one, 0)
        own_tile = tile_at(piece, own_u, own_v)
        own_place = own_u * 4 + own_v
        for slot in range(8):
            y_all[piece, own_place, slot] = y_near[piece, slot, own_tile]

    def send_sums(piece):
        own = place(piece, 1)
        for shift in (1, 3, 2):
            pltpu.make_async_remote_copy(
                src_ref=sums.at[piece, ring(own, shift)],
                dst_ref=sums_in.at[piece, shift - 1],
                send_sem=send_sem.at[1],
                recv_sem=sums_sem.at[piece],
                device_id=peer_of(piece, shift, 0),
                device_id_type=MESH,
            ).start()

    def send_series(piece):
        own_u, own_v = place(piece, 1), place(piece, 2)
        own_place = own_u * 4 + own_v
        for du, dv in OFFSETS:
            pltpu.make_async_remote_copy(
                src_ref=y_near.at[piece, :, tile_at(piece, ring(own_u, du), ring(own_v, dv))],
                dst_ref=y_all.at[piece, own_place],
                send_sem=send_sem.at[2],
                recv_sem=y_all_sem.at[piece],
                device_id=peer_of(piece, du, dv),
                device_id_type=MESH,
            ).start()

    def reduce_and_send(piece):
        await_bytes(sums_in.at[piece], sums_sem.at[piece])
        own_u, own_v = place(piece, 1), place(piece, 2)

        def one(v, carry):
            for i in range(5):
                part[piece, v, i] = (sums[piece, own_u, v, i] + sums_in[piece, 0, v, i]) + (
                    sums_in[piece, 1, v, i] + sums_in[piece, 2, v, i]
                )
            return carry

        lax.fori_loop(0, 4, one, 0)
        for shift in (1, 3, 2):
            pltpu.make_async_remote_copy(
                src_ref=part.at[piece, ring(own_v, shift)],
                dst_ref=part_in.at[piece, shift - 1],
                send_sem=send_sem.at[3],
                recv_sem=part_sem.at[piece],
                device_id=peer_of(piece, 0, shift),
                device_id_type=MESH,
            ).start()

    for piece in range(PIECES):
        await_bytes(y_near.at[piece], y_near_sem.at[piece])
        await_bytes(w_near.at[piece], w_near_sem.at[piece])
        partial_sums(piece)
        send_sums(piece)
        send_series(piece)
        if piece:
            reduce_and_send(piece - 1)
    reduce_and_send(PIECES - 1)

    def finish(piece):
        await_bytes(part_in.at[piece], part_sem.at[piece])
        own_v = place(piece, 2)
        s0, s1, s2, sy, sty = (
            (part[piece, own_v, i] + part_in[piece, 0, i]) + (part_in[piece, 1, i] + part_in[piece, 2, i])
            for i in range(5)
        )
        determinant = s0 * s2 - s1 * s1
        slope = (s0 * sty - s1 * sy) / determinant
        level = (s2 * sy - s1 * sty) / determinant
        columns = pl.ds(piece * LANES, LANES)
        fit[0, :, columns] = slope
        fit[1, :, columns] = level
        await_bytes(y_all.at[piece, pl.ds(0, 15)], y_all_sem.at[piece])

        def one(index, carry):
            u, v = lax.div(index, 4), lax.rem(index, 4)
            for slot in range(8):
                step = step_at(piece, slot, u, v)
                rest = y_all[piece, index, slot] - level - slope * centred_of(step)
                out[step, :, columns] = rest.astype(jnp.bfloat16)
            return carry

        lax.fori_loop(0, 16, one, 0)
        pltpu.make_async_copy(out.at[:, :, columns], anomaly_ref.at[:, :, columns], out_sem.at[piece]).start()

    for piece in range(PIECES):
        finish(piece)
    copies = [
        pltpu.make_async_copy(fit.at[0], slope_ref, out_sem.at[PIECES]),
        pltpu.make_async_copy(fit.at[1], level_ref, out_sem.at[PIECES + 1]),
    ]
    for copy in copies:
        copy.start()
    await_bytes(y_near.at[:, pl.ds(0, 7)], send_sem.at[0])
    await_bytes(w_near.at[:, pl.ds(0, 7)], send_sem.at[0])
    await_bytes(sums_in, send_sem.at[1])
    await_bytes(y_all.at[:, pl.ds(0, 15)], send_sem.at[2])
    await_bytes(part_in, send_sem.at[3])
    for piece in range(PIECES):
        columns = pl.ds(piece * LANES, LANES)
        pltpu.make_async_copy(out.at[:, :, columns], anomaly_ref.at[:, :, columns], out_sem.at[piece]).wait()
    for copy in copies:
        copy.wait()


def body(pixel_stack, quality_weight):
    def tiles(field):
        split = field.reshape(2, 4, 2, 8, 2, 4, PIECES, LANES)
        return split.transpose(0, 1, 2, 4, 5, 6, 3, 7)

    f32 = jnp.float32
    tile = (8, LANES)
    return pl.pallas_call(
        kernel,
        out_shape=(
            jax.ShapeDtypeStruct((8, 512), f32),
            jax.ShapeDtypeStruct((8, 512), f32),
            jax.ShapeDtypeStruct((128, 8, 512), jnp.bfloat16),
        ),
        in_specs=[pl.BlockSpec(memory_space=pl.ANY)] * 2,
        out_specs=(pl.BlockSpec(memory_space=pl.ANY),) * 3,
        scratch_shapes=[
            pltpu.VMEM((PIECES, 8, 16, *tile), f32),
            pltpu.VMEM((PIECES, 8, 16, *tile), f32),
            pltpu.VMEM((PIECES, 16, 8, *tile), f32),
            pltpu.VMEM((PIECES, 4, 4, 5, *tile), f32),
            pltpu.VMEM((PIECES, 3, 4, 5, *tile), f32),
            pltpu.VMEM((PIECES, 4, 5, *tile), f32),
            pltpu.VMEM((PIECES, 3, 5, *tile), f32),
            pltpu.VMEM((128, 8, 512), jnp.bfloat16),
            pltpu.VMEM((2, 8, 512), f32),
            pltpu.SemaphoreType.DMA((PIECES,)),
            pltpu.SemaphoreType.DMA((PIECES,)),
            pltpu.SemaphoreType.DMA((PIECES,)),
            pltpu.SemaphoreType.DMA((PIECES,)),
            pltpu.SemaphoreType.DMA((PIECES,)),
            pltpu.SemaphoreType.DMA((4,)),
            pltpu.SemaphoreType.DMA((PIECES + 2,)),
            pltpu.SemaphoreType.REGULAR,
        ],
        compiler_params=pltpu.CompilerParams(collective_id=0, has_side_effects=True),
    )(tiles(pixel_stack), tiles(quality_weight))


def solution(mesh):
    return jax.shard_map(
        body,
        mesh=mesh,
        in_specs=(P(("wide", "narrow"), None, None), P(("wide", "narrow"), None, None)),
        out_specs=(P("wide", "narrow"), P("wide", "narrow"), P(None, "wide", "narrow")),
        check_vma=False,
    )
```

```python
import jax
import jax.numpy as jnp
from jax import lax
from jax.experimental import pallas as pl
from jax.experimental.pallas import tpu as pltpu
from jax.sharding import PartitionSpec as P

MESH = pl.DeviceIdType.MESH
PIECES = 4
LANES = 128
ORDERS = (
    ("xzy", "yzx"),
    ("zyx", "xzy"),
    ("yxz", "zyx"),
    ("xzy", "yxz"),
)
OFFSETS = tuple((u, v) for u in (1, 3, 2, 0) for v in (1, 3, 2, 0) if (u, v) != (0, 0))
OFFSETS = OFFSETS[::4] + OFFSETS[1::4] + OFFSETS[2::4] + OFFSETS[3::4]
VIEWS = {"x": (4, 4), "y": (2, 4, 2), "z": (2, 2, 4)}


def ring(value, shift):
    return lax.rem(value + shift, 4)


def x_parts(x):
    return lax.rem(x, 2), lax.div(x, 2)


def device_of(at, core):
    low, high = x_parts(at["x"])
    return {"wide": low * 8 + at["z"] * 2 + core, "narrow": high * 4 + at["y"]}


def step_of(at, core):
    device = device_of(at, core)
    return device["wide"] * 8 + device["narrow"]


def tile_in_plane(first, at):
    low, high = x_parts(at["x"])
    if first == "x":
        return at["z"] * 4 + at["y"]
    if first == "y":
        return low * 8 + at["z"] * 2 + high
    return low * 8 + high * 4 + at["y"]


def kernel(
    y_ref, w_ref, slope_ref, level_ref, anomaly_ref,
    y_near, w_near, y_all, sums, sums_in, part, part_in,
    y_near_sem, w_near_sem, y_all_sem, sums_sem, part_sem, send_sem, ready_sem,
):
    wide, narrow = lax.axis_index("wide"), lax.axis_index("narrow")
    core = lax.rem(wide, 2)
    here = {
        "x": lax.div(narrow, 4) * 2 + lax.div(wide, 8),
        "y": lax.rem(narrow, 4),
        "z": lax.rem(lax.div(wide, 2), 4),
    }

    def select(values):
        zero, one = values
        return zero + core * (one - zero)

    def moved(**places):
        return {**here, **places}

    def by_core(function):
        return select([function(c) for c in range(2)])

    def peer_of(piece, shift_second, shift_third):
        places = []
        for c in range(2):
            _, second, third = ORDERS[piece][c]
            at = moved(**{second: ring(here[second], shift_second), third: ring(here[third], shift_third)})
            places.append(device_of(at, c))
        return {axis: select([place[axis] for place in places]) for axis in places[0]}

    def tile_at(piece, u, v):
        def of(c):
            first, second, third = ORDERS[piece][c]
            return tile_in_plane(first, moved(**{second: u, third: v}))

        return by_core(of)

    def place(piece, level):
        return by_core(lambda c: here[ORDERS[piece][c][level]])

    def step_at(piece, slot, u, v):
        def of(c):
            first, second, third = ORDERS[piece][c]
            return step_of(moved(**{first: slot // 2, second: u, third: v}), slot % 2)

        return by_core(of)

    def centred_of(step):
        return (step.astype(jnp.float32) - 63.5) * (1.0 / 128.0)

    barrier = pltpu.get_barrier_semaphore()
    count = 0
    for axis in "xyz":
        for shift in (1, 2, 3):
            for flip in range(2):
                target = device_of(moved(**{axis: ring(here[axis], shift)}), lax.rem(core + flip, 2))
                pl.semaphore_signal(barrier, inc=1, device_id=target, device_id_type=MESH)
                count += 1
    pl.semaphore_signal(barrier, inc=1, device_id=device_of(here, 1 - core), device_id_type=MESH)
    pl.semaphore_wait(barrier, count + 1)

    queues = {"x": [], "y": [], "z": []}
    for piece in range(PIECES):
        for c in range(2):
            first = ORDERS[piece][c][0]
            queues[first] += [(piece, c, shift) for shift in (1, 3, 2, 0)]

    def send_near(piece, c, shift):
        first = ORDERS[piece][c][0]
        where = ring(here[first], shift)
        low, high = x_parts(where)
        slot = here[first] * 2 + core
        for field, near, sem in ((y_ref, y_near, y_near_sem), (w_ref, w_near, w_near_sem)):
            if first == "x":
                source = field.at[low, :, c, high, :, piece]
            elif first == "y":
                source = field.at[:, :, c, :, where, piece]
            else:
                source = field.at[:, where, c, :, :, piece]
            target = near.at[piece, slot].reshape(*VIEWS[first], 8, LANES)

            def remote():
                pltpu.make_async_remote_copy(
                    src_ref=source,
                    dst_ref=target,
                    send_sem=send_sem.at[0],
                    recv_sem=sem.at[piece],
                    device_id=device_of(moved(**{first: where}), c),
                    device_id_type=MESH,
                ).start()

            if shift:
                remote()
            else:

                @pl.when(core == c)
                def _():
                    pltpu.make_async_copy(source, target, sem.at[piece]).start()

                pl.when(core != c)(remote)

    for turn in range(max(len(queue) for queue in queues.values())):
        for axis in "xyz":
            if turn < len(queues[axis]):
                send_near(*queues[axis][turn])

    for axis in "xyz":
        for shift in (1, 2, 3):
            target = device_of(moved(**{axis: ring(here[axis], shift)}), core)
            pl.semaphore_signal(ready_sem, inc=1, device_id=target, device_id_type=MESH)
    pl.semaphore_wait(ready_sem, 9)

    def await_bytes(ref, sem):
        pltpu.make_async_copy(ref, ref, sem).wait()

    def partial_sums(piece):
        own_u, own_v = place(piece, 1), place(piece, 2)
        centred = [centred_of(step_at(piece, slot, own_u, own_v)) for slot in range(8)]

        def one(index, carry):
            u, v = lax.div(index, 4), lax.rem(index, 4)
            tile = tile_at(piece, u, v)
            zero = jnp.zeros((8, LANES), jnp.float32)
            s0, s1, s2, sy, sty = zero, zero, zero, zero, zero
            for slot in range(8):
                w = w_near[piece, slot, tile]
                weighted = w * y_near[piece, slot, tile]
                moment = w * centred[slot]
                s0 += w
                s1 += moment
                s2 += moment * centred[slot]
                sy += weighted
                sty += weighted * centred[slot]
            for i, value in enumerate((s0, s1, s2, sy, sty)):
                sums[piece, u, v, i] = value
            return carry

        lax.fori_loop(0, 16, one, 0)
        own_tile = tile_at(piece, own_u, own_v)
        own_place = own_u * 4 + own_v
        for slot in range(8):
            y_all[piece, own_place, slot] = y_near[piece, slot, own_tile]

    def send_sums(piece):
        own = place(piece, 1)
        for shift in (1, 3, 2):
            pltpu.make_async_remote_copy(
                src_ref=sums.at[piece, ring(own, shift)],
                dst_ref=sums_in.at[piece, shift - 1],
                send_sem=send_sem.at[1],
                recv_sem=sums_sem.at[piece],
                device_id=peer_of(piece, shift, 0),
                device_id_type=MESH,
            ).start()

    def send_series(piece):
        own_u, own_v = place(piece, 1), place(piece, 2)
        own_place = own_u * 4 + own_v
        for du, dv in OFFSETS:
            pltpu.make_async_remote_copy(
                src_ref=y_near.at[piece, :, tile_at(piece, ring(own_u, du), ring(own_v, dv))],
                dst_ref=y_all.at[piece, own_place],
                send_sem=send_sem.at[2],
                recv_sem=y_all_sem.at[piece],
                device_id=peer_of(piece, du, dv),
                device_id_type=MESH,
            ).start()

    def reduce_and_send(piece):
        await_bytes(sums_in.at[piece], sums_sem.at[piece])
        own_u, own_v = place(piece, 1), place(piece, 2)

        def one(v, carry):
            for i in range(5):
                part[piece, v, i] = (sums[piece, own_u, v, i] + sums_in[piece, 0, v, i]) + (
                    sums_in[piece, 1, v, i] + sums_in[piece, 2, v, i]
                )
            return carry

        lax.fori_loop(0, 4, one, 0)
        for shift in (1, 3, 2):
            pltpu.make_async_remote_copy(
                src_ref=part.at[piece, ring(own_v, shift)],
                dst_ref=part_in.at[piece, shift - 1],
                send_sem=send_sem.at[3],
                recv_sem=part_sem.at[piece],
                device_id=peer_of(piece, 0, shift),
                device_id_type=MESH,
            ).start()

    for piece in range(PIECES):
        await_bytes(y_near.at[piece], y_near_sem.at[piece])
        await_bytes(w_near.at[piece], w_near_sem.at[piece])
        partial_sums(piece)
        send_sums(piece)
        send_series(piece)
    for piece in range(PIECES):
        reduce_and_send(piece)

    def finish(piece):
        await_bytes(part_in.at[piece], part_sem.at[piece])
        own_v = place(piece, 2)
        s0, s1, s2, sy, sty = (
            (part[piece, own_v, i] + part_in[piece, 0, i]) + (part_in[piece, 1, i] + part_in[piece, 2, i])
            for i in range(5)
        )
        determinant = s0 * s2 - s1 * s1
        slope = (s0 * sty - s1 * sy) / determinant
        level = (s2 * sy - s1 * sty) / determinant
        columns = pl.ds(piece * LANES, LANES)
        slope_ref[:, columns] = slope
        level_ref[:, columns] = level
        await_bytes(y_all.at[piece, pl.ds(0, 15)], y_all_sem.at[piece])

        def one(index, carry):
            u, v = lax.div(index, 4), lax.rem(index, 4)
            for slot in range(8):
                step = step_at(piece, slot, u, v)
                rest = y_all[piece, index, slot] - level - slope * centred_of(step)
                anomaly_ref[step, :, columns] = rest.astype(jnp.bfloat16)
            return carry

        lax.fori_loop(0, 16, one, 0)

    for piece in range(PIECES):
        finish(piece)
    await_bytes(y_near.at[:, pl.ds(0, 7)], send_sem.at[0])
    await_bytes(w_near.at[:, pl.ds(0, 7)], send_sem.at[0])
    await_bytes(sums_in, send_sem.at[1])
    await_bytes(y_all.at[:, pl.ds(0, 15)], send_sem.at[2])
    await_bytes(part_in, send_sem.at[3])


def body(pixel_stack, quality_weight):
    def tiles(field):
        split = field.reshape(2, 4, 2, 8, 2, 4, PIECES, LANES)
        return split.transpose(0, 1, 2, 4, 5, 6, 3, 7)

    f32 = jnp.float32
    tile = (8, LANES)
    return pl.pallas_call(
        kernel,
        out_shape=(
            pltpu.VMEM((8, 512), f32),
            pltpu.VMEM((8, 512), f32),
            pltpu.VMEM((128, 8, 512), jnp.bfloat16),
        ),
        in_specs=[pl.BlockSpec(memory_space=pl.ANY)] * 2,
        out_specs=(pl.BlockSpec(memory_space=pltpu.VMEM),) * 3,
        scratch_shapes=[
            pltpu.VMEM((PIECES, 8, 16, *tile), f32),
            pltpu.VMEM((PIECES, 8, 16, *tile), f32),
            pltpu.VMEM((PIECES, 16, 8, *tile), f32),
            pltpu.VMEM((PIECES, 4, 4, 5, *tile), f32),
            pltpu.VMEM((PIECES, 3, 4, 5, *tile), f32),
            pltpu.VMEM((PIECES, 4, 5, *tile), f32),
            pltpu.VMEM((PIECES, 3, 5, *tile), f32),
            pltpu.SemaphoreType.DMA((PIECES,)),
            pltpu.SemaphoreType.DMA((PIECES,)),
            pltpu.SemaphoreType.DMA((PIECES,)),
            pltpu.SemaphoreType.DMA((PIECES,)),
            pltpu.SemaphoreType.DMA((PIECES,)),
            pltpu.SemaphoreType.DMA((4,)),
            pltpu.SemaphoreType.REGULAR,
        ],
        compiler_params=pltpu.CompilerParams(collective_id=0, has_side_effects=True),
    )(tiles(pixel_stack), tiles(quality_weight))


def solution(mesh):
    return jax.shard_map(
        body,
        mesh=mesh,
        in_specs=(P(("wide", "narrow"), None, None), P(("wide", "narrow"), None, None)),
        out_specs=(P("wide", "narrow"), P("wide", "narrow"), P(None, "wide", "narrow")),
        check_vma=False,
    )
```

```python
import jax
import jax.numpy as jnp
from jax import lax
from jax.experimental import pallas as pl
from jax.experimental.pallas import tpu as pltpu
from jax.sharding import PartitionSpec as P

MESH = pl.DeviceIdType.MESH
PIECES = 4
LANES = 128
ORDERS = (
    ("xzy", "yzx"),
    ("zyx", "xzy"),
    ("yxz", "zyx"),
    ("xzy", "yxz"),
)
OFFSETS = tuple((u, v) for u in (1, 3, 2, 0) for v in (1, 3, 2, 0) if (u, v) != (0, 0))
OFFSETS = OFFSETS[::4] + OFFSETS[1::4] + OFFSETS[2::4] + OFFSETS[3::4]
SCHEDULE = "G0 G1 Y0 G2 Y1 G3 Y2 Y3 B0 B1 B2 B3 F0 F1 F2 F3"
VIEWS = {"x": (4, 4), "y": (2, 4, 2), "z": (2, 2, 4)}


def ring(value, shift):
    return lax.rem(value + shift, 4)


def x_parts(x):
    return lax.rem(x, 2), lax.div(x, 2)


def device_of(at, core):
    low, high = x_parts(at["x"])
    return {"wide": low * 8 + at["z"] * 2 + core, "narrow": high * 4 + at["y"]}


def step_of(at, core):
    device = device_of(at, core)
    return device["wide"] * 8 + device["narrow"]


def tile_in_plane(first, at):
    low, high = x_parts(at["x"])
    if first == "x":
        return at["z"] * 4 + at["y"]
    if first == "y":
        return low * 8 + at["z"] * 2 + high
    return low * 8 + high * 4 + at["y"]


def kernel(
    y_ref, w_ref, slope_ref, level_ref, anomaly_ref,
    y_near, w_near, y_all, sums, sums_in, part, part_in,
    y_near_sem, w_near_sem, y_all_sem, sums_sem, part_sem, send_sem, ready_sem,
):
    wide, narrow = lax.axis_index("wide"), lax.axis_index("narrow")
    core = lax.rem(wide, 2)
    here = {
        "x": lax.div(narrow, 4) * 2 + lax.div(wide, 8),
        "y": lax.rem(narrow, 4),
        "z": lax.rem(lax.div(wide, 2), 4),
    }

    def select(values):
        zero, one = values
        return zero + core * (one - zero)

    def moved(**places):
        return {**here, **places}

    def by_core(function):
        return select([function(c) for c in range(2)])

    def peer_of(piece, shift_second, shift_third):
        places = []
        for c in range(2):
            _, second, third = ORDERS[piece][c]
            at = moved(**{second: ring(here[second], shift_second), third: ring(here[third], shift_third)})
            places.append(device_of(at, c))
        return {axis: select([place[axis] for place in places]) for axis in places[0]}

    def tile_at(piece, u, v):
        def of(c):
            first, second, third = ORDERS[piece][c]
            return tile_in_plane(first, moved(**{second: u, third: v}))

        return by_core(of)

    def place(piece, level):
        return by_core(lambda c: here[ORDERS[piece][c][level]])

    def step_at(piece, slot, u, v):
        def of(c):
            first, second, third = ORDERS[piece][c]
            return step_of(moved(**{first: slot // 2, second: u, third: v}), slot % 2)

        return by_core(of)

    def centred_of(step):
        return (step.astype(jnp.float32) - 63.5) * (1.0 / 128.0)

    barrier = pltpu.get_barrier_semaphore()
    count = 0
    for axis in "xyz":
        for shift in (1, 2, 3):
            for flip in range(2):
                target = device_of(moved(**{axis: ring(here[axis], shift)}), lax.rem(core + flip, 2))
                pl.semaphore_signal(barrier, inc=1, device_id=target, device_id_type=MESH)
                count += 1
    pl.semaphore_signal(barrier, inc=1, device_id=device_of(here, 1 - core), device_id_type=MESH)
    pl.semaphore_wait(barrier, count + 1)

    queues = {"x": [], "y": [], "z": []}
    for piece in range(PIECES):
        for c in range(2):
            first = ORDERS[piece][c][0]
            queues[first] += [(piece, c, shift) for shift in (1, 3, 2, 0)]

    def send_near(piece, c, shift):
        first = ORDERS[piece][c][0]
        where = ring(here[first], shift)
        low, high = x_parts(where)
        slot = here[first] * 2 + core
        for field, near, sem in ((y_ref, y_near, y_near_sem), (w_ref, w_near, w_near_sem)):
            if first == "x":
                source = field.at[low, :, c, high, :, piece]
            elif first == "y":
                source = field.at[:, :, c, :, where, piece]
            else:
                source = field.at[:, where, c, :, :, piece]
            target = near.at[piece, slot].reshape(*VIEWS[first], 8, LANES)

            def remote():
                pltpu.make_async_remote_copy(
                    src_ref=source,
                    dst_ref=target,
                    send_sem=send_sem.at[0],
                    recv_sem=sem.at[piece],
                    device_id=device_of(moved(**{first: where}), c),
                    device_id_type=MESH,
                ).start()

            if shift:
                remote()
            else:

                @pl.when(core == c)
                def _():
                    pltpu.make_async_copy(source, target, sem.at[piece]).start()

                pl.when(core != c)(remote)

    for turn in range(max(len(queue) for queue in queues.values())):
        for axis in "xyz":
            if turn < len(queues[axis]):
                send_near(*queues[axis][turn])

    for axis in "xyz":
        for shift in (1, 2, 3):
            target = device_of(moved(**{axis: ring(here[axis], shift)}), core)
            pl.semaphore_signal(ready_sem, inc=1, device_id=target, device_id_type=MESH)
    pl.semaphore_wait(ready_sem, 9)

    def await_bytes(ref, sem):
        pltpu.make_async_copy(ref, ref, sem).wait()

    def partial_sums(piece):
        own_u, own_v = place(piece, 1), place(piece, 2)
        centred = [centred_of(step_at(piece, slot, own_u, own_v)) for slot in range(8)]

        def one(index, carry):
            u, v = lax.div(index, 4), lax.rem(index, 4)
            tile = tile_at(piece, u, v)
            zero = jnp.zeros((8, LANES), jnp.float32)
            s0, s1, s2, sy, sty = zero, zero, zero, zero, zero
            for slot in range(8):
                w = w_near[piece, slot, tile]
                weighted = w * y_near[piece, slot, tile]
                moment = w * centred[slot]
                s0 += w
                s1 += moment
                s2 += moment * centred[slot]
                sy += weighted
                sty += weighted * centred[slot]
            for i, value in enumerate((s0, s1, s2, sy, sty)):
                sums[piece, u, v, i] = value
            return carry

        lax.fori_loop(0, 16, one, 0)
        own_tile = tile_at(piece, own_u, own_v)
        own_place = own_u * 4 + own_v
        for slot in range(8):
            y_all[piece, own_place, slot] = y_near[piece, slot, own_tile]

    def send_sums(piece):
        own = place(piece, 1)
        for shift in (1, 3, 2):
            pltpu.make_async_remote_copy(
                src_ref=sums.at[piece, ring(own, shift)],
                dst_ref=sums_in.at[piece, shift - 1],
                send_sem=send_sem.at[1],
                recv_sem=sums_sem.at[piece],
                device_id=peer_of(piece, shift, 0),
                device_id_type=MESH,
            ).start()

    def send_series(piece):
        own_u, own_v = place(piece, 1), place(piece, 2)
        own_place = own_u * 4 + own_v
        for du, dv in OFFSETS:
            pltpu.make_async_remote_copy(
                src_ref=y_near.at[piece, :, tile_at(piece, ring(own_u, du), ring(own_v, dv))],
                dst_ref=y_all.at[piece, own_place],
                send_sem=send_sem.at[2],
                recv_sem=y_all_sem.at[piece],
                device_id=peer_of(piece, du, dv),
                device_id_type=MESH,
            ).start()

    def reduce_and_send(piece):
        await_bytes(sums_in.at[piece], sums_sem.at[piece])
        own_u, own_v = place(piece, 1), place(piece, 2)

        def one(v, carry):
            for i in range(5):
                part[piece, v, i] = (sums[piece, own_u, v, i] + sums_in[piece, 0, v, i]) + (
                    sums_in[piece, 1, v, i] + sums_in[piece, 2, v, i]
                )
            return carry

        lax.fori_loop(0, 4, one, 0)
        for shift in (1, 3, 2):
            pltpu.make_async_remote_copy(
                src_ref=part.at[piece, ring(own_v, shift)],
                dst_ref=part_in.at[piece, shift - 1],
                send_sem=send_sem.at[3],
                recv_sem=part_sem.at[piece],
                device_id=peer_of(piece, 0, shift),
                device_id_type=MESH,
            ).start()

    def gather(piece):
        await_bytes(y_near.at[piece], y_near_sem.at[piece])
        await_bytes(w_near.at[piece], w_near_sem.at[piece])
        partial_sums(piece)
        send_sums(piece)

    def finish(piece):
        await_bytes(part_in.at[piece], part_sem.at[piece])
        own_v = place(piece, 2)
        s0, s1, s2, sy, sty = (
            (part[piece, own_v, i] + part_in[piece, 0, i]) + (part_in[piece, 1, i] + part_in[piece, 2, i])
            for i in range(5)
        )
        determinant = s0 * s2 - s1 * s1
        slope = (s0 * sty - s1 * sy) / determinant
        level = (s2 * sy - s1 * sty) / determinant
        columns = pl.ds(piece * LANES, LANES)
        slope_ref[:, columns] = slope
        level_ref[:, columns] = level
        await_bytes(y_all.at[piece, pl.ds(0, 15)], y_all_sem.at[piece])

        start = step_at(piece, 0, 0, 0)
        ahead = [step_at(piece, slot, 0, 0) - start for slot in range(8)]
        trend = [slope * centred_of(start + shift) for shift in ahead]

        def one(index, carry):
            first_step = step_at(piece, 0, lax.div(index, 4), lax.rem(index, 4))
            rise = slope * ((first_step - start).astype(jnp.float32) * (1.0 / 128.0))
            for slot in range(8):
                rest = (y_all[piece, index, slot] - level) - (trend[slot] + rise)
                anomaly_ref[first_step + ahead[slot], :, columns] = rest.astype(jnp.bfloat16)
            return carry

        lax.fori_loop(0, 16, one, 0)

    phases = {"G": gather, "Y": send_series, "B": reduce_and_send, "F": finish}
    for name in SCHEDULE.split():
        phases[name[0]](int(name[1]))
    await_bytes(y_near.at[:, pl.ds(0, 7)], send_sem.at[0])
    await_bytes(w_near.at[:, pl.ds(0, 7)], send_sem.at[0])
    await_bytes(sums_in, send_sem.at[1])
    await_bytes(y_all.at[:, pl.ds(0, 15)], send_sem.at[2])
    await_bytes(part_in, send_sem.at[3])


def store(slope_ref, level_ref, anomaly_ref, slope_out, level_out, anomaly_out, sem):
    pairs = ((anomaly_ref, anomaly_out), (slope_ref, slope_out), (level_ref, level_out))
    copies = [pltpu.make_async_copy(source, target, sem.at[i]) for i, (source, target) in enumerate(pairs)]
    for copy in copies:
        copy.start()
    for copy in copies:
        copy.wait()


def body(pixel_stack, quality_weight):
    def tiles(field):
        split = field.reshape(2, 4, 2, 8, 2, 4, PIECES, LANES)
        return split.transpose(0, 1, 2, 4, 5, 6, 3, 7)

    f32 = jnp.float32
    tile = (8, LANES)
    fitted = pl.pallas_call(
        kernel,
        out_shape=(
            pltpu.VMEM((8, 512), f32),
            pltpu.VMEM((8, 512), f32),
            pltpu.VMEM((128, 8, 512), jnp.bfloat16),
        ),
        in_specs=[pl.BlockSpec(memory_space=pl.ANY)] * 2,
        out_specs=(pl.BlockSpec(memory_space=pltpu.VMEM),) * 3,
        scratch_shapes=[
            pltpu.VMEM((PIECES, 8, 16, *tile), f32),
            pltpu.VMEM((PIECES, 8, 16, *tile), f32),
            pltpu.VMEM((PIECES, 16, 8, *tile), f32),
            pltpu.VMEM((PIECES, 4, 4, 5, *tile), f32),
            pltpu.VMEM((PIECES, 3, 4, 5, *tile), f32),
            pltpu.VMEM((PIECES, 4, 5, *tile), f32),
            pltpu.VMEM((PIECES, 3, 5, *tile), f32),
            pltpu.SemaphoreType.DMA((PIECES,)),
            pltpu.SemaphoreType.DMA((PIECES,)),
            pltpu.SemaphoreType.DMA((PIECES,)),
            pltpu.SemaphoreType.DMA((PIECES,)),
            pltpu.SemaphoreType.DMA((PIECES,)),
            pltpu.SemaphoreType.DMA((4,)),
            pltpu.SemaphoreType.REGULAR,
        ],
        compiler_params=pltpu.CompilerParams(collective_id=0, has_side_effects=True),
    )(tiles(pixel_stack), tiles(quality_weight))
    return pl.pallas_call(
        store,
        out_shape=tuple(jax.ShapeDtypeStruct(field.shape, field.dtype) for field in fitted),
        in_specs=[pl.BlockSpec(memory_space=pltpu.VMEM)] * 3,
        out_specs=(pl.BlockSpec(memory_space=pl.ANY),) * 3,
        scratch_shapes=[pltpu.SemaphoreType.DMA((3,))],
    )(*(pltpu.with_memory_space_constraint(field, pltpu.VMEM) for field in fitted))


def solution(mesh):
    return jax.shard_map(
        body,
        mesh=mesh,
        in_specs=(P(("wide", "narrow"), None, None), P(("wide", "narrow"), None, None)),
        out_specs=(P("wide", "narrow"), P("wide", "narrow"), P(None, "wide", "narrow")),
        check_vma=False,
    )
```

```python
import functools

import jax
import jax.numpy as jnp
from jax import lax
from jax.experimental import pallas as pl
from jax.experimental.pallas import tpu as pltpu
from jax.sharding import PartitionSpec as P

MESH = pl.DeviceIdType.MESH
PIECES = 4
LANES = 128
ORDERS = (("xzy", "yzx"), ("zyx", "xzy"), ("yxz", "zyx"), ("xzy", "yxz"))
OFFSETS = ((0, 0), (0, 1), (1, 0), (0, None), (None, 0), (0, 2), (1, 1), (2, 0), (None, 1), (1, None), (1, 2), (2, 1), (None, 2), (2, None), (2, 2))
TURNS = ((0, 0), (0, 1), (1, 0), (1, 1), (2, 0), (2, 1), (None, 0), (None, 1))
SCHEDULE = ("S0S1S2S3", "R", "G0", "G1", "Y0", "G2", "Y1", "G3", "Y2", "P3", "B0", "B1", "B2", "B3", "Q3", "F0", "F1", "F2", "F3")
VIEWS = {"x": (4, 4), "y": (2, 4, 2), "z": (2, 2, 4)}


def ring(value, shift):
    return lax.rem(value + shift, 4)


def x_parts(x):
    return lax.rem(x, 2), lax.div(x, 2)


def device_of(at, core):
    low, high = x_parts(at["x"])
    return {"wide": low * 8 + at["z"] * 2 + core, "narrow": high * 4 + at["y"]}


def step_of(at, core):
    device = device_of(at, core)
    return device["wide"] * 8 + device["narrow"]


def tile_in_plane(first, at):
    low, high = x_parts(at["x"])
    if first == "x":
        return at["z"] * 4 + at["y"]
    if first == "y":
        return low * 8 + at["z"] * 2 + high
    return low * 8 + high * 4 + at["y"]


def kernel(
    y_ref, w_ref, slope_ref, level_ref, anomaly_ref,
    y_near, w_near, y_all, sums, sums_in, part, part_in,
    y_near_sem, w_near_sem, y_all_sem, sums_sem, part_sem, send_sem, seen_sem, ready_sem,
):
    wide, narrow = lax.axis_index("wide"), lax.axis_index("narrow")
    core = lax.rem(wide, 2)
    here = {
        "x": lax.div(narrow, 4) * 2 + lax.div(wide, 8),
        "y": lax.rem(narrow, 4),
        "z": lax.rem(lax.div(wide, 2), 4),
    }

    def select(values):
        zero, one = values
        return zero + core * (one - zero)

    def moved(**places):
        return {**here, **places}

    def by_core(function):
        return select([function(c) for c in range(2)])

    def peer_of(piece, shift_second, shift_third):
        places = []
        for c in range(2):
            _, second, third = ORDERS[piece][c]
            at = moved(**{second: ring(here[second], shift_second), third: ring(here[third], shift_third)})
            places.append(device_of(at, c))
        return {axis: select([place[axis] for place in places]) for axis in places[0]}

    def tile_at(piece, u, v):
        def of(c):
            first, second, third = ORDERS[piece][c]
            return tile_in_plane(first, moved(**{second: u, third: v}))

        return by_core(of)

    def place(piece, level):
        return by_core(lambda c: here[ORDERS[piece][c][level]])

    def step_at(piece, slot, u, v):
        def of(c):
            first, second, third = ORDERS[piece][c]
            return step_of(moved(**{first: slot // 2, second: u, third: v}), slot % 2)

        return by_core(of)

    def centred_of(step):
        return (step.astype(jnp.float32) - 63.5) * (1.0 / 128.0)

    barrier = pltpu.get_barrier_semaphore()

    def greet(condition, semaphore, target):
        @pl.when(condition)
        def _():
            pl.semaphore_signal(semaphore, inc=1, device_id=target, device_id_type=MESH)

    everyone = [(n, axis, q, c) for n, axis in enumerate("xyz") for q in range(4) for c in range(2)]
    for _, axis, q, c in everyone:
        greet(here[axis] < q, barrier, device_of(moved(**{axis: q}), c))
    greet(core == 1, barrier, device_of(here, 0))
    before = 2 * (here["x"] + here["y"] + here["z"]) + (1 - core)

    @pl.when(before > 0)
    def _():
        pl.semaphore_wait(barrier, before)

    for n, axis, q, c in everyone:
        greet(q < here[axis], seen_sem.at[8 * n + 2 * here[axis] + core], device_of(moved(**{axis: q}), c))
    greet(core == 0, seen_sem.at[24], device_of(here, 1))
    heard = set()

    def hear(condition, key, index):
        if key not in heard:
            heard.add(key)

            @pl.when(condition)
            def _():
                pl.semaphore_wait(seen_sem.at[index], 1)

    def mirrored(shift):
        return shift

    def near_copy(piece, c, shift, which):
        first = ORDERS[piece][c][0]
        where = here[first] if shift is None else nth(here[first], shift)
        low, high = x_parts(where)
        field, near, sem = ((y_ref, y_near, y_near_sem), (w_ref, w_near, w_near_sem))[which]
        if first == "x":
            source = field.at[low, :, c, high, :, piece]
        elif first == "y":
            source = field.at[:, :, c, :, where, piece]
        else:
            source = field.at[:, where, c, :, :, piece]
        target = near.at[piece, here[first] * 2 + core].reshape(*VIEWS[first], 8, LANES)

        def remote():
            pltpu.make_async_remote_copy(
                src_ref=source,
                dst_ref=target,
                send_sem=send_sem.at[0],
                recv_sem=sem.at[piece],
                device_id=device_of(moved(**{first: where}), c),
                device_id_type=MESH,
            ).start()

        if shift is not None:
            hear(here[first] <= shift, (first, shift, c), 8 * "xyz".index(first) + 2 * where + c)
            remote()
        else:

            @pl.when(core == c)
            def _():
                pltpu.make_async_copy(source, target, sem.at[piece]).start()

            if c == 0:
                hear(core == 1, c, 24)
            pl.when(core != c)(remote)

    def nth(own, k):
        return own if k is None else k + (own <= k).astype(jnp.int32)

    def near_copies(pieces):
        queues = {"x": [], "y": [], "z": []}
        for piece in pieces:
            for shift, which in ((0, 0), (0, 1), (1, 0), (1, 1), (2, 0), (2, 1), (None, 0), (None, 1)):
                for c in range(2):
                    queues[ORDERS[piece][c][0]].append(functools.partial(near_copy, piece, c, shift, which))
        return merge([queue for queue in queues.values() if queue])

    def merge(lists):
        ranked = [((i + 0.5) / len(items), n, item) for n, items in enumerate(lists) for i, item in enumerate(items)]
        return [item for _, _, item in sorted(ranked, key=lambda entry: entry[:2])]

    def await_partners():
        for axis in "xyz":
            for shift in (1, 2, 3):
                target = device_of(moved(**{axis: ring(here[axis], shift)}), core)
                pl.semaphore_signal(ready_sem, inc=1, device_id=target, device_id_type=MESH)
        pl.semaphore_wait(ready_sem, 9)

    def await_bytes(ref, sem):
        pltpu.make_async_copy(ref, ref, sem).wait()

    def partial_sums(piece):
        own_u, own_v = place(piece, 1), place(piece, 2)
        centred = [centred_of(step_at(piece, slot, own_u, own_v)) for slot in range(8)]

        def one(index, carry):
            u, v = lax.div(index, 4), lax.rem(index, 4)
            tile = tile_at(piece, u, v)
            zero = jnp.zeros((8, LANES), jnp.float32)
            s0, s1, s2, sy, sty = zero, zero, zero, zero, zero
            for slot in range(8):
                w = w_near[piece, slot, tile]
                weighted = w * y_near[piece, slot, tile]
                moment = w * centred[slot]
                s0 += w
                s1 += moment
                s2 += moment * centred[slot]
                sy += weighted
                sty += weighted * centred[slot]
            for i, value in enumerate((s0, s1, s2, sy, sty)):
                sums[piece, u, v, i] = value
            return carry

        lax.fori_loop(0, 16, one, 0)
        own_tile = tile_at(piece, own_u, own_v)
        own_place = own_u * 4 + own_v
        for slot in range(8):
            y_all[piece, own_place, slot] = y_near[piece, slot, own_tile]

    def send_sums(piece):
        own = place(piece, 1)
        for n in range(3):
            u = nth(own, n)
            pltpu.make_async_remote_copy(
                src_ref=sums.at[piece, u],
                dst_ref=sums_in.at[piece, own - (u < own).astype(jnp.int32)],
                send_sem=send_sem.at[1],
                recv_sem=sums_sem.at[piece],
                device_id=peer_of(piece, u - own + 4, 0),
                device_id_type=MESH,
            ).start()

    def series_copy(piece, du, dv):
        own_u, own_v = place(piece, 1), place(piece, 2)
        u, v = nth(own_u, du), nth(own_v, dv)
        pltpu.make_async_remote_copy(
            src_ref=y_near.at[piece, :, tile_at(piece, u, v)],
            dst_ref=y_all.at[piece, own_u * 4 + own_v],
            send_sem=send_sem.at[2],
            recv_sem=y_all_sem.at[piece],
            device_id=peer_of(piece, u - own_u + 4, v - own_v + 4),
            device_id_type=MESH,
        ).start()

    def series_copies(kind, piece):
        part = {"Y": OFFSETS, "P": OFFSETS[:11], "Q": OFFSETS[11:]}[kind]
        return [functools.partial(series_copy, piece, du, dv) for du, dv in part]

    def reduce_and_send(piece):
        await_bytes(sums_in.at[piece], sums_sem.at[piece])
        own_u, own_v = place(piece, 1), place(piece, 2)

        def one(v, carry):
            for i in range(5):
                part[piece, v, i] = (sums[piece, own_u, v, i] + sums_in[piece, 0, v, i]) + (
                    sums_in[piece, 1, v, i] + sums_in[piece, 2, v, i]
                )
            return carry

        lax.fori_loop(0, 4, one, 0)
        for n in range(3):
            v = nth(own_v, n)
            pltpu.make_async_remote_copy(
                src_ref=part.at[piece, v],
                dst_ref=part_in.at[piece, own_v - (v < own_v).astype(jnp.int32)],
                send_sem=send_sem.at[3],
                recv_sem=part_sem.at[piece],
                device_id=peer_of(piece, 0, v - own_v + 4),
                device_id_type=MESH,
            ).start()

    def gather(piece):
        await_bytes(y_near.at[piece], y_near_sem.at[piece])
        await_bytes(w_near.at[piece], w_near_sem.at[piece])
        partial_sums(piece)
        send_sums(piece)

    def finish(piece):
        await_bytes(part_in.at[piece], part_sem.at[piece])
        own_v = place(piece, 2)
        s0, s1, s2, sy, sty = (
            (part[piece, own_v, i] + part_in[piece, 0, i]) + (part_in[piece, 1, i] + part_in[piece, 2, i])
            for i in range(5)
        )
        determinant = s0 * s2 - s1 * s1
        slope = (s0 * sty - s1 * sy) / determinant
        level = (s2 * sy - s1 * sty) / determinant
        columns = pl.ds(piece * LANES, LANES)
        slope_ref[:, columns] = slope
        level_ref[:, columns] = level
        await_bytes(y_all.at[piece, pl.ds(0, 15)], y_all_sem.at[piece])

        start = step_at(piece, 0, 0, 0)
        ahead = [step_at(piece, slot, 0, 0) - start for slot in range(8)]
        trend = [slope * centred_of(start + shift) for shift in ahead]

        def one(index, carry):
            first_step = step_at(piece, 0, lax.div(index, 4), lax.rem(index, 4))
            rise = slope * ((first_step - start).astype(jnp.float32) * (1.0 / 128.0))
            for slot in range(8):
                rest = (y_all[piece, index, slot] - level) - (trend[slot] + rise)
                anomaly_ref[first_step + ahead[slot], :, columns] = rest.astype(jnp.bfloat16)
            return carry

        lax.fori_loop(0, 16, one, 0)

    steps = {"G": gather, "B": reduce_and_send, "F": finish}
    for name in SCHEDULE:
        if name == "R":
            await_partners()
        elif name[0] in steps:
            steps[name[0]](int(name[1]))
        else:
            pairs = [(name[i], int(name[i + 1])) for i in range(0, len(name), 2)]
            near = [piece for kind, piece in pairs if kind == "S"]
            lists = [near_copies(near)] if near else []
            for copy in merge(lists + [series_copies(kind, piece) for kind, piece in pairs if kind != "S"]):
                copy()

    await_bytes(y_near.at[:, pl.ds(0, 7)], send_sem.at[0])
    await_bytes(w_near.at[:, pl.ds(0, 7)], send_sem.at[0])
    await_bytes(sums_in, send_sem.at[1])
    await_bytes(y_all.at[:, pl.ds(0, 15)], send_sem.at[2])
    await_bytes(part_in, send_sem.at[3])


def store(slope_ref, level_ref, anomaly_ref, slope_out, level_out, anomaly_out, sem):
    pairs = ((anomaly_ref, anomaly_out), (slope_ref, slope_out), (level_ref, level_out))
    copies = [pltpu.make_async_copy(source, target, sem.at[i]) for i, (source, target) in enumerate(pairs)]
    for copy in copies:
        copy.start()
    for copy in copies:
        copy.wait()


def body(pixel_stack, quality_weight):
    def tiles(field):
        split = field.reshape(2, 4, 2, 8, 2, 4, PIECES, LANES)
        return split.transpose(0, 1, 2, 4, 5, 6, 3, 7)

    f32 = jnp.float32
    tile = (8, LANES)
    fitted = pl.pallas_call(
        kernel,
        out_shape=(
            pltpu.VMEM((8, 512), f32),
            pltpu.VMEM((8, 512), f32),
            pltpu.VMEM((128, 8, 512), jnp.bfloat16),
        ),
        in_specs=[pl.BlockSpec(memory_space=pl.ANY)] * 2,
        out_specs=(pl.BlockSpec(memory_space=pltpu.VMEM),) * 3,
        scratch_shapes=[
            pltpu.VMEM((PIECES, 8, 16, *tile), f32),
            pltpu.VMEM((PIECES, 8, 16, *tile), f32),
            pltpu.VMEM((PIECES, 16, 8, *tile), f32),
            pltpu.VMEM((PIECES, 4, 4, 5, *tile), f32),
            pltpu.VMEM((PIECES, 3, 4, 5, *tile), f32),
            pltpu.VMEM((PIECES, 4, 5, *tile), f32),
            pltpu.VMEM((PIECES, 3, 5, *tile), f32),
            pltpu.SemaphoreType.DMA((PIECES,)),
            pltpu.SemaphoreType.DMA((PIECES,)),
            pltpu.SemaphoreType.DMA((PIECES,)),
            pltpu.SemaphoreType.DMA((PIECES,)),
            pltpu.SemaphoreType.DMA((PIECES,)),
            pltpu.SemaphoreType.DMA((4,)),
            pltpu.SemaphoreType.REGULAR((25,)),
            pltpu.SemaphoreType.REGULAR,
        ],
        compiler_params=pltpu.CompilerParams(collective_id=0, has_side_effects=True),
    )(tiles(pixel_stack), tiles(quality_weight))
    return pl.pallas_call(
        store,
        out_shape=tuple(jax.ShapeDtypeStruct(field.shape, field.dtype) for field in fitted),
        in_specs=[pl.BlockSpec(memory_space=pltpu.VMEM)] * 3,
        out_specs=(pl.BlockSpec(memory_space=pl.ANY),) * 3,
        scratch_shapes=[pltpu.SemaphoreType.DMA((3,))],
    )(*(pltpu.with_memory_space_constraint(field, pltpu.VMEM) for field in fitted))


def solution(mesh):
    return jax.shard_map(
        body,
        mesh=mesh,
        in_specs=(P(("wide", "narrow"), None, None), P(("wide", "narrow"), None, None)),
        out_specs=(P("wide", "narrow"), P("wide", "narrow"), P(None, "wide", "narrow")),
        check_vma=False,
    )
```

```python
import functools

import jax
import jax.numpy as jnp
from jax import lax
from jax.experimental import pallas as pl
from jax.experimental.pallas import tpu as pltpu
from jax.sharding import PartitionSpec as P

MESH = pl.DeviceIdType.MESH
PIECES = 4
LANES = 128
ORDERS = (("xzy", "yzx"), ("zyx", "xzy"), ("yxz", "zyx"), ("xzy", "yxz"))
OFFSETS = ((0, 0), (0, 1), (1, 0), (0, None), (None, 0), (0, 2), (1, 1), (2, 0), (None, 1), (1, None), (1, 2), (2, 1), (None, 2), (2, None), (2, 2))
TURNS = ((0, 0), (0, 1), (1, 0), (1, 1), (2, 0), (2, 1), (None, 0), (None, 1))
SCHEDULE = ("S0S1S2", "R", "S3", "G0", "G1", "Y0", "G2", "Y1", "G3", "Y2", "P3", "B0", "B1", "B2", "B3", "Q3", "F0", "F1", "F2", "F3")
VIEWS = {"x": (4, 4), "y": (2, 4, 2), "z": (2, 2, 4)}


def ring(value, shift):
    return lax.rem(value + shift, 4)


def x_parts(x):
    return lax.rem(x, 2), lax.div(x, 2)


def device_of(at, core):
    low, high = x_parts(at["x"])
    return {"wide": low * 8 + at["z"] * 2 + core, "narrow": high * 4 + at["y"]}


def step_of(at, core):
    device = device_of(at, core)
    return device["wide"] * 8 + device["narrow"]


def tile_in_plane(first, at):
    low, high = x_parts(at["x"])
    if first == "x":
        return at["z"] * 4 + at["y"]
    if first == "y":
        return low * 8 + at["z"] * 2 + high
    return low * 8 + high * 4 + at["y"]


def kernel(
    y_ref, w_ref, slope_ref, level_ref, anomaly_ref,
    y_near, w_near, y_all, sums, sums_in, part, part_in,
    y_near_sem, w_near_sem, y_all_sem, sums_sem, part_sem, send_sem, seen_sem, ready_sem,
):
    wide, narrow = lax.axis_index("wide"), lax.axis_index("narrow")
    core = lax.rem(wide, 2)
    here = {
        "x": lax.div(narrow, 4) * 2 + lax.div(wide, 8),
        "y": lax.rem(narrow, 4),
        "z": lax.rem(lax.div(wide, 2), 4),
    }

    def select(values):
        zero, one = values
        return zero + core * (one - zero)

    def moved(**places):
        return {**here, **places}

    def by_core(function):
        return select([function(c) for c in range(2)])

    def peer_of(piece, shift_second, shift_third):
        places = []
        for c in range(2):
            _, second, third = ORDERS[piece][c]
            at = moved(**{second: ring(here[second], shift_second), third: ring(here[third], shift_third)})
            places.append(device_of(at, c))
        return {axis: select([place[axis] for place in places]) for axis in places[0]}

    def tile_at(piece, u, v):
        def of(c):
            first, second, third = ORDERS[piece][c]
            return tile_in_plane(first, moved(**{second: u, third: v}))

        return by_core(of)

    def place(piece, level):
        return by_core(lambda c: here[ORDERS[piece][c][level]])

    def step_at(piece, slot, u, v):
        def of(c):
            first, second, third = ORDERS[piece][c]
            return step_of(moved(**{first: slot // 2, second: u, third: v}), slot % 2)

        return by_core(of)

    def centred_of(step):
        return (step.astype(jnp.float32) - 63.5) * (1.0 / 128.0)

    barrier = pltpu.get_barrier_semaphore()

    def greet(condition, semaphore, target):
        @pl.when(condition)
        def _():
            pl.semaphore_signal(semaphore, inc=1, device_id=target, device_id_type=MESH)

    everyone = [(n, axis, q, c) for n, axis in enumerate("xyz") for q in range(4) for c in range(2)]
    for _, axis, q, c in everyone:
        greet(here[axis] < q, barrier, device_of(moved(**{axis: q}), c))
    greet(core == 1, barrier, device_of(here, 0))
    before = 2 * (here["x"] + here["y"] + here["z"]) + (1 - core)

    @pl.when(before > 0)
    def _():
        pl.semaphore_wait(barrier, before)

    for n, axis, q, c in everyone:
        greet(q < here[axis], seen_sem.at[8 * n + 2 * here[axis] + core], device_of(moved(**{axis: q}), c))
    greet(core == 0, seen_sem.at[24], device_of(here, 1))
    heard = set()

    def hear(condition, key, index):
        if key not in heard:
            heard.add(key)

            @pl.when(condition)
            def _():
                pl.semaphore_wait(seen_sem.at[index], 1)

    def mirrored(shift):
        return shift

    def near_copy(piece, c, shift, which):
        first = ORDERS[piece][c][0]
        where = here[first] if shift is None else nth(here[first], shift)
        low, high = x_parts(where)
        field, near, sem = ((y_ref, y_near, y_near_sem), (w_ref, w_near, w_near_sem))[which]
        if first == "x":
            source = field.at[low, :, c, high, :, piece]
        elif first == "y":
            source = field.at[:, :, c, :, where, piece]
        else:
            source = field.at[:, where, c, :, :, piece]
        target = near.at[piece, here[first] * 2 + core].reshape(*VIEWS[first], 8, LANES)

        def remote():
            pltpu.make_async_remote_copy(
                src_ref=source,
                dst_ref=target,
                send_sem=send_sem.at[0],
                recv_sem=sem.at[piece],
                device_id=device_of(moved(**{first: where}), c),
                device_id_type=MESH,
            ).start()

        if shift is not None:
            hear(here[first] <= shift, (first, shift, c), 8 * "xyz".index(first) + 2 * where + c)
            remote()
        else:

            @pl.when(core == c)
            def _():
                pltpu.make_async_copy(source, target, sem.at[piece]).start()

            if c == 0:
                hear(core == 1, c, 24)
            pl.when(core != c)(remote)

    def nth(own, k):
        return own if k is None else k + (own <= k).astype(jnp.int32)

    def near_copies(pieces):
        queues = {"x": [], "y": [], "z": []}
        for piece in pieces:
            for shift, which in ((0, 0), (0, 1), (1, 0), (1, 1), (2, 0), (2, 1), (None, 0), (None, 1)):
                for c in range(2):
                    queues[ORDERS[piece][c][0]].append(functools.partial(near_copy, piece, c, shift, which))
        return merge([queue for queue in queues.values() if queue])

    def merge(lists):
        ranked = [((i + 0.5) / len(items), n, item) for n, items in enumerate(lists) for i, item in enumerate(items)]
        return [item for _, _, item in sorted(ranked, key=lambda entry: entry[:2])]

    def await_partners():
        for axis in "xyz":
            for shift in (1, 2, 3):
                target = device_of(moved(**{axis: ring(here[axis], shift)}), core)
                pl.semaphore_signal(ready_sem, inc=1, device_id=target, device_id_type=MESH)
        pl.semaphore_wait(ready_sem, 9)

    def await_bytes(ref, sem):
        pltpu.make_async_copy(ref, ref, sem).wait()

    def partial_sums(piece):
        own_u, own_v = place(piece, 1), place(piece, 2)
        centred = [centred_of(step_at(piece, slot, own_u, own_v)) for slot in range(8)]

        def one(index, carry):
            u, v = lax.div(index, 4), lax.rem(index, 4)
            tile = tile_at(piece, u, v)
            zero = jnp.zeros((8, LANES), jnp.float32)
            s0, s1, s2, sy, sty = zero, zero, zero, zero, zero
            for slot in range(8):
                w = w_near[piece, slot, tile]
                weighted = w * y_near[piece, slot, tile]
                moment = w * centred[slot]
                s0 += w
                s1 += moment
                s2 += moment * centred[slot]
                sy += weighted
                sty += weighted * centred[slot]
            for i, value in enumerate((s0, s1, s2, sy, sty)):
                sums[piece, u, v, i] = value
            return carry

        lax.fori_loop(0, 16, one, 0)
        own_tile = tile_at(piece, own_u, own_v)
        own_place = own_u * 4 + own_v
        for slot in range(8):
            y_all[piece, own_place, slot] = y_near[piece, slot, own_tile]

    def send_sums(piece):
        own = place(piece, 1)
        for n in range(3):
            u = nth(own, n)
            pltpu.make_async_remote_copy(
                src_ref=sums.at[piece, u],
                dst_ref=sums_in.at[piece, own - (u < own).astype(jnp.int32)],
                send_sem=send_sem.at[1],
                recv_sem=sums_sem.at[piece],
                device_id=peer_of(piece, u - own + 4, 0),
                device_id_type=MESH,
            ).start()

    def series_copy(piece, du, dv):
        own_u, own_v = place(piece, 1), place(piece, 2)
        u, v = nth(own_u, du), nth(own_v, dv)
        pltpu.make_async_remote_copy(
            src_ref=y_near.at[piece, :, tile_at(piece, u, v)],
            dst_ref=y_all.at[piece, own_u * 4 + own_v],
            send_sem=send_sem.at[2],
            recv_sem=y_all_sem.at[piece],
            device_id=peer_of(piece, u - own_u + 4, v - own_v + 4),
            device_id_type=MESH,
        ).start()

    def series_copies(kind, piece):
        part = {"Y": OFFSETS, "P": OFFSETS[:11], "Q": OFFSETS[11:]}[kind]
        return [functools.partial(series_copy, piece, du, dv) for du, dv in part]

    def reduce_and_send(piece):
        await_bytes(sums_in.at[piece], sums_sem.at[piece])
        own_u, own_v = place(piece, 1), place(piece, 2)

        def one(v, carry):
            for i in range(5):
                part[piece, v, i] = (sums[piece, own_u, v, i] + sums_in[piece, 0, v, i]) + (
                    sums_in[piece, 1, v, i] + sums_in[piece, 2, v, i]
                )
            return carry

        lax.fori_loop(0, 4, one, 0)
        for n in range(3):
            v = nth(own_v, n)
            pltpu.make_async_remote_copy(
                src_ref=part.at[piece, v],
                dst_ref=part_in.at[piece, own_v - (v < own_v).astype(jnp.int32)],
                send_sem=send_sem.at[3],
                recv_sem=part_sem.at[piece],
                device_id=peer_of(piece, 0, v - own_v + 4),
                device_id_type=MESH,
            ).start()

    def gather(piece):
        await_bytes(y_near.at[piece], y_near_sem.at[piece])
        await_bytes(w_near.at[piece], w_near_sem.at[piece])
        partial_sums(piece)
        send_sums(piece)

    def finish(piece):
        await_bytes(part_in.at[piece], part_sem.at[piece])
        own_v = place(piece, 2)
        s0, s1, s2, sy, sty = (
            (part[piece, own_v, i] + part_in[piece, 0, i]) + (part_in[piece, 1, i] + part_in[piece, 2, i])
            for i in range(5)
        )
        determinant = s0 * s2 - s1 * s1
        slope = (s0 * sty - s1 * sy) / determinant
        level = (s2 * sy - s1 * sty) / determinant
        columns = pl.ds(piece * LANES, LANES)
        slope_ref[:, columns] = slope
        level_ref[:, columns] = level
        await_bytes(y_all.at[piece, pl.ds(0, 15)], y_all_sem.at[piece])

        start = step_at(piece, 0, 0, 0)
        ahead = [step_at(piece, slot, 0, 0) - start for slot in range(8)]
        trend = [slope * centred_of(start + shift) for shift in ahead]

        def one(index, carry):
            first_step = step_at(piece, 0, lax.div(index, 4), lax.rem(index, 4))
            rise = slope * ((first_step - start).astype(jnp.float32) * (1.0 / 128.0))
            for slot in range(8):
                rest = (y_all[piece, index, slot] - level) - (trend[slot] + rise)
                anomaly_ref[first_step + ahead[slot], :, columns] = rest.astype(jnp.bfloat16)
            return carry

        lax.fori_loop(0, 16, one, 0)

    steps = {"G": gather, "B": reduce_and_send, "F": finish}
    for name in SCHEDULE:
        if name == "R":
            await_partners()
        elif name[0] in steps:
            steps[name[0]](int(name[1]))
        else:
            pairs = [(name[i], int(name[i + 1])) for i in range(0, len(name), 2)]
            near = [piece for kind, piece in pairs if kind == "S"]
            lists = [near_copies(near)] if near else []
            for copy in merge(lists + [series_copies(kind, piece) for kind, piece in pairs if kind != "S"]):
                copy()

    await_bytes(y_near.at[:, pl.ds(0, 7)], send_sem.at[0])
    await_bytes(w_near.at[:, pl.ds(0, 7)], send_sem.at[0])
    await_bytes(sums_in, send_sem.at[1])
    await_bytes(y_all.at[:, pl.ds(0, 15)], send_sem.at[2])
    await_bytes(part_in, send_sem.at[3])


def store(slope_ref, level_ref, anomaly_ref, slope_out, level_out, anomaly_out, sem):
    pairs = ((anomaly_ref, anomaly_out), (slope_ref, slope_out), (level_ref, level_out))
    copies = [pltpu.make_async_copy(source, target, sem.at[i]) for i, (source, target) in enumerate(pairs)]
    for copy in copies:
        copy.start()
    for copy in copies:
        copy.wait()


def body(pixel_stack, quality_weight):
    def tiles(field):
        split = field.reshape(2, 4, 2, 8, 2, 4, PIECES, LANES)
        return split.transpose(0, 1, 2, 4, 5, 6, 3, 7)

    f32 = jnp.float32
    tile = (8, LANES)
    fitted = pl.pallas_call(
        kernel,
        out_shape=(
            pltpu.VMEM((8, 512), f32),
            pltpu.VMEM((8, 512), f32),
            pltpu.VMEM((128, 8, 512), jnp.bfloat16),
        ),
        in_specs=[pl.BlockSpec(memory_space=pl.ANY)] * 2,
        out_specs=(pl.BlockSpec(memory_space=pltpu.VMEM),) * 3,
        scratch_shapes=[
            pltpu.VMEM((PIECES, 8, 16, *tile), f32),
            pltpu.VMEM((PIECES, 8, 16, *tile), f32),
            pltpu.VMEM((PIECES, 16, 8, *tile), f32),
            pltpu.VMEM((PIECES, 4, 4, 5, *tile), f32),
            pltpu.VMEM((PIECES, 3, 4, 5, *tile), f32),
            pltpu.VMEM((PIECES, 4, 5, *tile), f32),
            pltpu.VMEM((PIECES, 3, 5, *tile), f32),
            pltpu.SemaphoreType.DMA((PIECES,)),
            pltpu.SemaphoreType.DMA((PIECES,)),
            pltpu.SemaphoreType.DMA((PIECES,)),
            pltpu.SemaphoreType.DMA((PIECES,)),
            pltpu.SemaphoreType.DMA((PIECES,)),
            pltpu.SemaphoreType.DMA((4,)),
            pltpu.SemaphoreType.REGULAR((25,)),
            pltpu.SemaphoreType.REGULAR,
        ],
        compiler_params=pltpu.CompilerParams(collective_id=0, has_side_effects=True),
    )(tiles(pixel_stack), tiles(quality_weight))
    return pl.pallas_call(
        store,
        out_shape=tuple(jax.ShapeDtypeStruct(field.shape, field.dtype) for field in fitted),
        in_specs=[pl.BlockSpec(memory_space=pltpu.VMEM)] * 3,
        out_specs=(pl.BlockSpec(memory_space=pl.ANY),) * 3,
        scratch_shapes=[pltpu.SemaphoreType.DMA((3,))],
    )(*(pltpu.with_memory_space_constraint(field, pltpu.VMEM) for field in fitted))


def solution(mesh):
    return jax.shard_map(
        body,
        mesh=mesh,
        in_specs=(P(("wide", "narrow"), None, None), P(("wide", "narrow"), None, None)),
        out_specs=(P("wide", "narrow"), P("wide", "narrow"), P(None, "wide", "narrow")),
        check_vma=False,
    )
```

```python
import functools

import jax
import jax.numpy as jnp
from jax import lax
from jax.experimental import pallas as pl
from jax.experimental.pallas import tpu as pltpu
from jax.sharding import PartitionSpec as P

MESH = pl.DeviceIdType.MESH
PIECES = 4
LANES = 128
ORDERS = (("xzy", "yzx"), ("zyx", "xzy"), ("yxz", "zyx"), ("xzy", "yxz"))
OFFSETS = ((0, 0), (0, 1), (1, 0), (0, None), (None, 0), (0, 2), (1, 1), (2, 0), (None, 1), (1, None), (1, 2), (2, 1), (None, 2), (2, None), (2, 2))
TURNS = ((0, 0), (0, 1), (1, 0), (1, 1), (2, 0), (2, 1), (None, 0), (None, 1))
SCHEDULE = ("S0S1S2", "R", "S3", "G0", "G1", "Y0", "G2", "Y1", "G3", "Y2", "P3", "B0", "B1", "B2", "B3", "Q3", "F0", "F1", "F2", "F3")
VIEWS = {"x": (4, 4), "y": (2, 4, 2), "z": (2, 2, 4)}


def ring(value, shift):
    return lax.rem(value + shift, 4)


def x_parts(x):
    return lax.rem(x, 2), lax.div(x, 2)


def device_of(at, core):
    low, high = x_parts(at["x"])
    return {"wide": low * 8 + at["z"] * 2 + core, "narrow": high * 4 + at["y"]}


def step_of(at, core):
    device = device_of(at, core)
    return device["wide"] * 8 + device["narrow"]


def tile_in_plane(first, at):
    low, high = x_parts(at["x"])
    if first == "x":
        return at["z"] * 4 + at["y"]
    if first == "y":
        return low * 8 + at["z"] * 2 + high
    return low * 8 + high * 4 + at["y"]


def kernel(
    y_ref, w_ref, slope_ref, level_ref, anomaly_ref,
    y_near, w_near, y_all, sums, sums_in, part, part_in,
    y_near_sem, w_near_sem, y_all_sem, sums_sem, part_sem, send_sem, seen_sem, ready_sem,
):
    wide, narrow = lax.axis_index("wide"), lax.axis_index("narrow")
    core = lax.rem(wide, 2)
    here = {
        "x": lax.div(narrow, 4) * 2 + lax.div(wide, 8),
        "y": lax.rem(narrow, 4),
        "z": lax.rem(lax.div(wide, 2), 4),
    }

    def select(values):
        zero, one = values
        return zero + core * (one - zero)

    def moved(**places):
        return {**here, **places}

    def by_core(function):
        return select([function(c) for c in range(2)])

    def peer_of(piece, shift_second, shift_third):
        places = []
        for c in range(2):
            _, second, third = ORDERS[piece][c]
            at = moved(**{second: ring(here[second], shift_second), third: ring(here[third], shift_third)})
            places.append(device_of(at, c))
        return {axis: select([place[axis] for place in places]) for axis in places[0]}

    def tile_at(piece, u, v):
        def of(c):
            first, second, third = ORDERS[piece][c]
            return tile_in_plane(first, moved(**{second: u, third: v}))

        return by_core(of)

    def place(piece, level):
        return by_core(lambda c: here[ORDERS[piece][c][level]])

    def step_at(piece, slot, u, v):
        def of(c):
            first, second, third = ORDERS[piece][c]
            return step_of(moved(**{first: slot // 2, second: u, third: v}), slot % 2)

        return by_core(of)

    def centred_of(step):
        return (step.astype(jnp.float32) - 63.5) * (1.0 / 128.0)

    barrier = pltpu.get_barrier_semaphore()

    def greet(condition, semaphore, target):
        @pl.when(condition)
        def _():
            pl.semaphore_signal(semaphore, inc=1, device_id=target, device_id_type=MESH)

    everyone = [(n, axis, q, c) for n, axis in enumerate("xyz") for q in range(4) for c in range(2)]
    for _, axis, q, c in everyone:
        greet(here[axis] < q, barrier, device_of(moved(**{axis: q}), c))
    greet(core == 1, barrier, device_of(here, 0))
    before = 2 * (here["x"] + here["y"] + here["z"]) + (1 - core)

    @pl.when(before > 0)
    def _():
        pl.semaphore_wait(barrier, before)

    for n, axis, q, c in everyone:
        greet(q < here[axis], seen_sem.at[8 * n + 2 * here[axis] + core], device_of(moved(**{axis: q}), c))
    greet(core == 0, seen_sem.at[24], device_of(here, 1))
    heard, sender = set(), [0]

    def hear(condition, key, index):
        key = (sender[0], key)
        if key not in heard:
            heard.add(key)

            @pl.when(condition)
            def _():
                pl.semaphore_wait(seen_sem.at[index], 1)

    def mirrored(shift):
        return shift

    def near_copy(piece, c, shift, which):
        first = ORDERS[piece][c][0]
        where = here[first] if shift is None else nth(here[first], shift)
        low, high = x_parts(where)
        field, near, sem = ((y_ref, y_near, y_near_sem), (w_ref, w_near, w_near_sem))[which]
        if first == "x":
            source = field.at[low, :, c, high, :, piece]
        elif first == "y":
            source = field.at[:, :, c, :, where, piece]
        else:
            source = field.at[:, where, c, :, :, piece]
        target = near.at[piece, here[first] * 2 + core].reshape(*VIEWS[first], 8, LANES)

        def remote():
            pltpu.make_async_remote_copy(
                src_ref=source,
                dst_ref=target,
                send_sem=send_sem.at[0],
                recv_sem=sem.at[piece],
                device_id=device_of(moved(**{first: where}), c),
                device_id_type=MESH,
            ).start()

        if shift is not None:
            hear(here[first] <= shift, (first, shift, c), 8 * "xyz".index(first) + 2 * where + c)
            remote()
        else:

            @pl.when(core == c)
            def _():
                pltpu.make_async_copy(source, target, sem.at[piece]).start()

            if c == 0:
                hear(core == 1, c, 24)
            pl.when(core != c)(remote)

    def nth(own, k):
        return own if k is None else k + (own <= k).astype(jnp.int32)

    def near_copies(pieces):
        queues = {"x": [], "y": [], "z": []}
        for piece in pieces:
            for shift, which in ((0, 0), (0, 1), (1, 0), (1, 1), (2, 0), (2, 1), (None, 0), (None, 1)):
                for c in range(2):
                    queues[ORDERS[piece][c][0]].append(functools.partial(near_copy, piece, c, shift, which))
        lists = list(queues.values())
        turned = 2 * sender[0]
        return merge([queue for queue in lists[turned:] + lists[:turned] if queue])

    def merge(lists):
        ranked = [((i + 0.5) / len(items), n, item) for n, items in enumerate(lists) for i, item in enumerate(items)]
        return [item for _, _, item in sorted(ranked, key=lambda entry: entry[:2])]

    def await_partners():
        for axis in "xyz":
            for shift in (1, 2, 3):
                target = device_of(moved(**{axis: ring(here[axis], shift)}), core)
                pl.semaphore_signal(ready_sem, inc=1, device_id=target, device_id_type=MESH)
        pl.semaphore_wait(ready_sem, 9)

    def await_bytes(ref, sem):
        pltpu.make_async_copy(ref, ref, sem).wait()

    def partial_sums(piece):
        own_u, own_v = place(piece, 1), place(piece, 2)
        centred = [centred_of(step_at(piece, slot, own_u, own_v)) for slot in range(8)]

        def one(index, carry):
            u, v = lax.div(index, 4), lax.rem(index, 4)
            tile = tile_at(piece, u, v)
            zero = jnp.zeros((8, LANES), jnp.float32)
            s0, s1, s2, sy, sty = zero, zero, zero, zero, zero
            for slot in range(8):
                w = w_near[piece, slot, tile]
                weighted = w * y_near[piece, slot, tile]
                moment = w * centred[slot]
                s0 += w
                s1 += moment
                s2 += moment * centred[slot]
                sy += weighted
                sty += weighted * centred[slot]
            for i, value in enumerate((s0, s1, s2, sy, sty)):
                sums[piece, u, v, i] = value
            return carry

        lax.fori_loop(0, 16, one, 0)
        own_tile = tile_at(piece, own_u, own_v)
        own_place = own_u * 4 + own_v
        for slot in range(8):
            y_all[piece, own_place, slot] = y_near[piece, slot, own_tile]

    def send_sums(piece):
        own = place(piece, 1)
        for n in range(3):
            u = nth(own, n)
            pltpu.make_async_remote_copy(
                src_ref=sums.at[piece, u],
                dst_ref=sums_in.at[piece, own - (u < own).astype(jnp.int32)],
                send_sem=send_sem.at[1],
                recv_sem=sums_sem.at[piece],
                device_id=peer_of(piece, u - own + 4, 0),
                device_id_type=MESH,
            ).start()

    def series_copy(piece, du, dv):
        own_u, own_v = place(piece, 1), place(piece, 2)
        u, v = nth(own_u, du), nth(own_v, dv)
        pltpu.make_async_remote_copy(
            src_ref=y_near.at[piece, :, tile_at(piece, u, v)],
            dst_ref=y_all.at[piece, own_u * 4 + own_v],
            send_sem=send_sem.at[2],
            recv_sem=y_all_sem.at[piece],
            device_id=peer_of(piece, u - own_u + 4, v - own_v + 4),
            device_id_type=MESH,
        ).start()

    def series_copies(kind, piece):
        part = {"Y": OFFSETS, "P": OFFSETS[:11], "Q": OFFSETS[11:]}[kind]
        return [functools.partial(series_copy, piece, du, dv) for du, dv in part]

    def reduce_and_send(piece):
        await_bytes(sums_in.at[piece], sums_sem.at[piece])
        own_u, own_v = place(piece, 1), place(piece, 2)

        def one(v, carry):
            for i in range(5):
                part[piece, v, i] = (sums[piece, own_u, v, i] + sums_in[piece, 0, v, i]) + (
                    sums_in[piece, 1, v, i] + sums_in[piece, 2, v, i]
                )
            return carry

        lax.fori_loop(0, 4, one, 0)
        for n in range(3):
            v = nth(own_v, n)
            pltpu.make_async_remote_copy(
                src_ref=part.at[piece, v],
                dst_ref=part_in.at[piece, own_v - (v < own_v).astype(jnp.int32)],
                send_sem=send_sem.at[3],
                recv_sem=part_sem.at[piece],
                device_id=peer_of(piece, 0, v - own_v + 4),
                device_id_type=MESH,
            ).start()

    def gather(piece):
        await_bytes(y_near.at[piece], y_near_sem.at[piece])
        await_bytes(w_near.at[piece], w_near_sem.at[piece])
        partial_sums(piece)
        send_sums(piece)

    def finish(piece):
        await_bytes(part_in.at[piece], part_sem.at[piece])
        own_v = place(piece, 2)
        s0, s1, s2, sy, sty = (
            (part[piece, own_v, i] + part_in[piece, 0, i]) + (part_in[piece, 1, i] + part_in[piece, 2, i])
            for i in range(5)
        )
        determinant = s0 * s2 - s1 * s1
        slope = (s0 * sty - s1 * sy) / determinant
        level = (s2 * sy - s1 * sty) / determinant
        columns = pl.ds(piece * LANES, LANES)
        slope_ref[:, columns] = slope
        level_ref[:, columns] = level
        await_bytes(y_all.at[piece, pl.ds(0, 15)], y_all_sem.at[piece])

        start = step_at(piece, 0, 0, 0)
        ahead = [step_at(piece, slot, 0, 0) - start for slot in range(8)]
        trend = [slope * centred_of(start + shift) for shift in ahead]

        def one(index, carry):
            first_step = step_at(piece, 0, lax.div(index, 4), lax.rem(index, 4))
            rise = slope * ((first_step - start).astype(jnp.float32) * (1.0 / 128.0))
            for slot in range(8):
                rest = (y_all[piece, index, slot] - level) - (trend[slot] + rise)
                anomaly_ref[first_step + ahead[slot], :, columns] = rest.astype(jnp.bfloat16)
            return carry

        lax.fori_loop(0, 16, one, 0)

    steps = {"G": gather, "B": reduce_and_send, "F": finish}
    for name in SCHEDULE:
        if name == "R":
            await_partners()
        elif name[0] in steps:
            steps[name[0]](int(name[1]))
        else:
            pairs = [(name[i], int(name[i + 1])) for i in range(0, len(name), 2)]
            near = [piece for kind, piece in pairs if kind == "S"]
            if near:
                for sender[0] in range(2):

                    @pl.when(core == sender[0])
                    def _():
                        for copy in near_copies(near):
                            copy()

            for copy in merge([series_copies(kind, piece) for kind, piece in pairs if kind != "S"]):
                copy()

    await_bytes(y_near.at[:, pl.ds(0, 7)], send_sem.at[0])
    await_bytes(w_near.at[:, pl.ds(0, 7)], send_sem.at[0])
    await_bytes(sums_in, send_sem.at[1])
    await_bytes(y_all.at[:, pl.ds(0, 15)], send_sem.at[2])
    await_bytes(part_in, send_sem.at[3])


def store(slope_ref, level_ref, anomaly_ref, slope_out, level_out, anomaly_out, sem):
    pairs = ((anomaly_ref, anomaly_out), (slope_ref, slope_out), (level_ref, level_out))
    copies = [pltpu.make_async_copy(source, target, sem.at[i]) for i, (source, target) in enumerate(pairs)]
    for copy in copies:
        copy.start()
    for copy in copies:
        copy.wait()


def body(pixel_stack, quality_weight):
    def tiles(field):
        split = field.reshape(2, 4, 2, 8, 2, 4, PIECES, LANES)
        return split.transpose(0, 1, 2, 4, 5, 6, 3, 7)

    f32 = jnp.float32
    tile = (8, LANES)
    fitted = pl.pallas_call(
        kernel,
        out_shape=(
            pltpu.VMEM((8, 512), f32),
            pltpu.VMEM((8, 512), f32),
            pltpu.VMEM((128, 8, 512), jnp.bfloat16),
        ),
        in_specs=[pl.BlockSpec(memory_space=pl.ANY)] * 2,
        out_specs=(pl.BlockSpec(memory_space=pltpu.VMEM),) * 3,
        scratch_shapes=[
            pltpu.VMEM((PIECES, 8, 16, *tile), f32),
            pltpu.VMEM((PIECES, 8, 16, *tile), f32),
            pltpu.VMEM((PIECES, 16, 8, *tile), f32),
            pltpu.VMEM((PIECES, 4, 4, 5, *tile), f32),
            pltpu.VMEM((PIECES, 3, 4, 5, *tile), f32),
            pltpu.VMEM((PIECES, 4, 5, *tile), f32),
            pltpu.VMEM((PIECES, 3, 5, *tile), f32),
            pltpu.SemaphoreType.DMA((PIECES,)),
            pltpu.SemaphoreType.DMA((PIECES,)),
            pltpu.SemaphoreType.DMA((PIECES,)),
            pltpu.SemaphoreType.DMA((PIECES,)),
            pltpu.SemaphoreType.DMA((PIECES,)),
            pltpu.SemaphoreType.DMA((4,)),
            pltpu.SemaphoreType.REGULAR((25,)),
            pltpu.SemaphoreType.REGULAR,
        ],
        compiler_params=pltpu.CompilerParams(collective_id=0, has_side_effects=True),
    )(tiles(pixel_stack), tiles(quality_weight))
    return pl.pallas_call(
        store,
        out_shape=tuple(jax.ShapeDtypeStruct(field.shape, field.dtype) for field in fitted),
        in_specs=[pl.BlockSpec(memory_space=pltpu.VMEM)] * 3,
        out_specs=(pl.BlockSpec(memory_space=pl.ANY),) * 3,
        scratch_shapes=[pltpu.SemaphoreType.DMA((3,))],
    )(*(pltpu.with_memory_space_constraint(field, pltpu.VMEM) for field in fitted))


def solution(mesh):
    return jax.shard_map(
        body,
        mesh=mesh,
        in_specs=(P(("wide", "narrow"), None, None), P(("wide", "narrow"), None, None)),
        out_specs=(P("wide", "narrow"), P("wide", "narrow"), P(None, "wide", "narrow")),
        check_vma=False,
    )
```

```python
import functools

import jax
import jax.numpy as jnp
from jax import lax
from jax.experimental import pallas as pl
from jax.experimental.pallas import tpu as pltpu
from jax.sharding import PartitionSpec as P

MESH = pl.DeviceIdType.MESH
PIECES = 4
PARTS = 4
LANES = 128
ORDERS = (("xzy", "yzx"), ("zyx", "xzy"), ("yxz", "zyx"), ("xzy", "yxz"))
OFFSETS = ((0, 0), (0, 1), (1, 0), (0, None), (None, 0), (0, 2), (1, 1), (2, 0), (None, 1), (1, None), (1, 2), (2, 1), (None, 2), (2, None), (2, 2))
TURNS = ((0, 0), (0, 1), (1, 0), (1, 1), (2, 0), (2, 1), (None, 0), (None, 1))
SCHEDULE = ("S0S1S2", "R", "S3", "G0", "G1", "Y0", "G2", "Y1", "G3", "Y2", "P3", "B0", "B1", "B2", "B3", "Q3", "F0", "F1", "F2", "F3")
VIEWS = {"x": (4, 4), "y": (2, 4, 2), "z": (2, 2, 4)}


def ring(value, shift):
    return lax.rem(value + shift, 4)


def x_parts(x):
    return lax.rem(x, 2), lax.div(x, 2)


def device_of(at, core):
    low, high = x_parts(at["x"])
    return {"wide": low * 8 + at["z"] * 2 + core, "narrow": high * 4 + at["y"]}


def step_of(at, core):
    device = device_of(at, core)
    return device["wide"] * 8 + device["narrow"]


def tile_in_plane(first, at):
    low, high = x_parts(at["x"])
    if first == "x":
        return at["z"] * 4 + at["y"]
    if first == "y":
        return low * 8 + at["z"] * 2 + high
    return low * 8 + high * 4 + at["y"]


def kernel(
    y_ref, w_ref, slope_ref, level_ref, anomaly_ref,
    y_near, w_near, y_all, sums, sums_in, part, part_in,
    y_near_sem, w_near_sem, y_all_sem, sums_sem, part_sem, send_sem, seen_sem, ready_sem,
):
    wide, narrow = lax.axis_index("wide"), lax.axis_index("narrow")
    core = lax.rem(wide, 2)
    here = {
        "x": lax.div(narrow, 4) * 2 + lax.div(wide, 8),
        "y": lax.rem(narrow, 4),
        "z": lax.rem(lax.div(wide, 2), 4),
    }

    def select(values):
        zero, one = values
        return zero + core * (one - zero)

    def moved(**places):
        return {**here, **places}

    def by_core(function):
        return select([function(c) for c in range(2)])

    def peer_of(piece, shift_second, shift_third):
        places = []
        for c in range(2):
            _, second, third = ORDERS[piece][c]
            at = moved(**{second: ring(here[second], shift_second), third: ring(here[third], shift_third)})
            places.append(device_of(at, c))
        return {axis: select([place[axis] for place in places]) for axis in places[0]}

    def tile_at(piece, u, v):
        def of(c):
            first, second, third = ORDERS[piece][c]
            return tile_in_plane(first, moved(**{second: u, third: v}))

        return by_core(of)

    def place(piece, level):
        return by_core(lambda c: here[ORDERS[piece][c][level]])

    def step_at(piece, slot, u, v):
        def of(c):
            first, second, third = ORDERS[piece][c]
            return step_of(moved(**{first: slot // 2, second: u, third: v}), slot % 2)

        return by_core(of)

    def centred_of(step):
        return (step.astype(jnp.float32) - 63.5) * (1.0 / 128.0)

    barrier = pltpu.get_barrier_semaphore()

    def greet(condition, semaphore, target):
        @pl.when(condition)
        def _():
            pl.semaphore_signal(semaphore, inc=1, device_id=target, device_id_type=MESH)

    everyone = [(n, axis, q, c) for n, axis in enumerate("xyz") for q in range(4) for c in range(2)]
    for _, axis, q, c in everyone:
        greet(here[axis] < q, barrier, device_of(moved(**{axis: q}), c))
    greet(core == 1, barrier, device_of(here, 0))
    before = 2 * (here["x"] + here["y"] + here["z"]) + (1 - core)

    @pl.when(before > 0)
    def _():
        pl.semaphore_wait(barrier, before)

    for n, axis, q, c in everyone:
        greet(q < here[axis], seen_sem.at[8 * n + 2 * here[axis] + core], device_of(moved(**{axis: q}), c))
    greet(core == 0, seen_sem.at[24], device_of(here, 1))
    heard, sender = set(), [0]

    def hear(condition, key, index):
        key = (sender[0], key)
        if key not in heard:
            heard.add(key)

            @pl.when(condition)
            def _():
                pl.semaphore_wait(seen_sem.at[index], 1)

    def mirrored(shift):
        return shift

    def near_copy(piece, c, shift, which):
        first = ORDERS[piece][c][0]
        where = here[first] if shift is None else nth(here[first], shift)
        low, high = x_parts(where)
        field, near, sem = ((y_ref, y_near, y_near_sem), (w_ref, w_near, w_near_sem))[which]
        if first == "x":
            source = field.at[low, :, c, high, :, piece]
        elif first == "y":
            source = field.at[:, :, c, :, where, piece]
        else:
            source = field.at[:, where, c, :, :, piece]
        target = near.at[piece, here[first] * 2 + core].reshape(*VIEWS[first], 8, LANES)

        def remote():
            pltpu.make_async_remote_copy(
                src_ref=source,
                dst_ref=target,
                send_sem=send_sem.at[0],
                recv_sem=sem.at[piece],
                device_id=device_of(moved(**{first: where}), c),
                device_id_type=MESH,
            ).start()

        if shift is not None:
            hear(here[first] <= shift, (first, shift, c), 8 * "xyz".index(first) + 2 * where + c)
            remote()
        else:

            @pl.when(core == c)
            def _():
                pltpu.make_async_copy(source, target, sem.at[piece]).start()

            if c == 0:
                hear(core == 1, c, 24)
            pl.when(core != c)(remote)

    def nth(own, k):
        return own if k is None else k + (own <= k).astype(jnp.int32)

    def near_copies(pieces):
        queues = {"x": [], "y": [], "z": []}
        for piece in pieces:
            for shift, which in ((0, 0), (0, 1), (1, 0), (1, 1), (2, 0), (2, 1), (None, 0), (None, 1)):
                for c in range(2):
                    queues[ORDERS[piece][c][0]].append(functools.partial(near_copy, piece, c, shift, which))
        lists = list(queues.values())
        turned = 2 * sender[0]
        return merge([queue for queue in lists[turned:] + lists[:turned] if queue])

    def merge(lists):
        ranked = [((i + 0.5) / len(items), n, item) for n, items in enumerate(lists) for i, item in enumerate(items)]
        return [item for _, _, item in sorted(ranked, key=lambda entry: entry[:2])]

    def await_partners():
        for axis in "xyz":
            for shift in (1, 2, 3):
                target = device_of(moved(**{axis: ring(here[axis], shift)}), core)
                pl.semaphore_signal(ready_sem, inc=1, device_id=target, device_id_type=MESH)
        pl.semaphore_wait(ready_sem, 9)

    def await_bytes(ref, sem):
        pltpu.make_async_copy(ref, ref, sem).wait()

    def partial_sums(piece):
        own_u, own_v = place(piece, 1), place(piece, 2)
        centred = [centred_of(step_at(piece, slot, own_u, own_v)) for slot in range(8)]

        def one(index, carry):
            u, v = lax.div(index, 4), lax.rem(index, 4)
            tile = tile_at(piece, u, v)
            zero = jnp.zeros((8, LANES), jnp.float32)
            s0, s1, s2, sy, sty = zero, zero, zero, zero, zero
            for slot in range(8):
                w = w_near[piece, slot, tile]
                weighted = w * y_near[piece, slot, tile]
                moment = w * centred[slot]
                s0 += w
                s1 += moment
                s2 += moment * centred[slot]
                sy += weighted
                sty += weighted * centred[slot]
            for i, value in enumerate((s0, s1, s2, sy, sty)):
                sums[piece, u, v, i] = value
            return carry

        lax.fori_loop(0, 16, one, 0)
        own_tile = tile_at(piece, own_u, own_v)
        own_place = own_u * 4 + own_v
        for slot in range(8):
            y_all[piece, own_place, slot] = y_near[piece, slot, own_tile]

    def send_sums(piece):
        own = place(piece, 1)
        for n in range(3):
            u = nth(own, n)
            pltpu.make_async_remote_copy(
                src_ref=sums.at[piece, u],
                dst_ref=sums_in.at[piece, own - (u < own).astype(jnp.int32)],
                send_sem=send_sem.at[1],
                recv_sem=sums_sem.at[piece],
                device_id=peer_of(piece, u - own + 4, 0),
                device_id_type=MESH,
            ).start()

    def series_copy(piece, du, dv):
        own_u, own_v = place(piece, 1), place(piece, 2)
        u, v = nth(own_u, du), nth(own_v, dv)
        pltpu.make_async_remote_copy(
            src_ref=y_near.at[piece, :, tile_at(piece, u, v)],
            dst_ref=y_all.at[piece, own_u * 4 + own_v],
            send_sem=send_sem.at[2],
            recv_sem=y_all_sem.at[piece],
            device_id=peer_of(piece, u - own_u + 4, v - own_v + 4),
            device_id_type=MESH,
        ).start()

    def series_copies(kind, piece):
        part = {"Y": OFFSETS, "P": OFFSETS[:11], "Q": OFFSETS[11:]}[kind]
        return [functools.partial(series_copy, piece, du, dv) for du, dv in part]

    def reduce_and_send(piece):
        await_bytes(sums_in.at[piece], sums_sem.at[piece])
        own_u, own_v = place(piece, 1), place(piece, 2)

        def one(v, carry):
            for i in range(5):
                part[piece, v, i] = (sums[piece, own_u, v, i] + sums_in[piece, 0, v, i]) + (
                    sums_in[piece, 1, v, i] + sums_in[piece, 2, v, i]
                )
            return carry

        lax.fori_loop(0, 4, one, 0)
        for n in range(3):
            v = nth(own_v, n)
            pltpu.make_async_remote_copy(
                src_ref=part.at[piece, v],
                dst_ref=part_in.at[piece, own_v - (v < own_v).astype(jnp.int32)],
                send_sem=send_sem.at[3],
                recv_sem=part_sem.at[piece],
                device_id=peer_of(piece, 0, v - own_v + 4),
                device_id_type=MESH,
            ).start()

    def gather(piece):
        await_bytes(y_near.at[piece], y_near_sem.at[piece])
        await_bytes(w_near.at[piece], w_near_sem.at[piece])
        partial_sums(piece)
        send_sums(piece)

    def finish(piece):
        await_bytes(part_in.at[piece], part_sem.at[piece])
        own_v = place(piece, 2)
        s0, s1, s2, sy, sty = (
            (part[piece, own_v, i] + part_in[piece, 0, i]) + (part_in[piece, 1, i] + part_in[piece, 2, i])
            for i in range(5)
        )
        determinant = s0 * s2 - s1 * s1
        slope = (s0 * sty - s1 * sy) / determinant
        level = (s2 * sy - s1 * sty) / determinant
        columns = pl.ds(piece * LANES, LANES)
        slope_ref[:, columns] = slope
        level_ref[:, columns] = level
        await_bytes(y_all.at[piece, pl.ds(0, 15)], y_all_sem.at[piece])

        start = step_at(piece, 0, 0, 0)
        ahead = [step_at(piece, slot, 0, 0) - start for slot in range(8)]
        trend = [slope * centred_of(start + shift) for shift in ahead]

        def one(index, carry):
            first_step = step_at(piece, 0, lax.div(index, 4), lax.rem(index, 4))
            rise = slope * ((first_step - start).astype(jnp.float32) * (1.0 / 128.0))
            for slot in range(8):
                rest = (y_all[piece, index, slot] - level) - (trend[slot] + rise)
                anomaly_ref[first_step + ahead[slot], :, columns] = rest.astype(jnp.bfloat16)
            return carry

        lax.fori_loop(0, 16, one, 0)

    steps = {"G": gather, "B": reduce_and_send, "F": finish}
    for name in SCHEDULE:
        if name == "R":
            await_partners()
        elif name[0] in steps:
            steps[name[0]](int(name[1]))
        else:
            pairs = [(name[i], int(name[i + 1])) for i in range(0, len(name), 2)]
            near = [piece for kind, piece in pairs if kind == "S"]
            if near:
                for sender[0] in range(2):

                    @pl.when(core == sender[0])
                    def _():
                        for copy in near_copies(near):
                            copy()

            for copy in merge([series_copies(kind, piece) for kind, piece in pairs if kind != "S"]):
                copy()

    await_bytes(y_near.at[:, pl.ds(0, 7)], send_sem.at[0])
    await_bytes(w_near.at[:, pl.ds(0, 7)], send_sem.at[0])
    await_bytes(sums_in, send_sem.at[1])
    await_bytes(y_all.at[:, pl.ds(0, 15)], send_sem.at[2])
    await_bytes(part_in, send_sem.at[3])


def store(slope_ref, level_ref, anomaly_ref, slope_out, level_out, anomaly_out, sem):
    steps = anomaly_ref.shape[0] // PARTS
    pairs = [(slope_ref, slope_out), (level_ref, level_out)]
    for part in range(PARTS):
        rows = pl.ds(part * steps, steps)
        pairs.append((anomaly_ref.at[rows], anomaly_out.at[rows]))
    copies = [pltpu.make_async_copy(source, target, sem.at[i]) for i, (source, target) in enumerate(pairs)]
    for copy in copies:
        copy.start()
    for copy in copies:
        copy.wait()


def body(pixel_stack, quality_weight):
    def tiles(field):
        split = field.reshape(2, 4, 2, 8, 2, 4, PIECES, LANES)
        return split.transpose(0, 1, 2, 4, 5, 6, 3, 7)

    f32 = jnp.float32
    tile = (8, LANES)
    fitted = pl.pallas_call(
        kernel,
        out_shape=(
            pltpu.VMEM((8, 512), f32),
            pltpu.VMEM((8, 512), f32),
            pltpu.VMEM((128, 8, 512), jnp.bfloat16),
        ),
        in_specs=[pl.BlockSpec(memory_space=pl.ANY)] * 2,
        out_specs=(pl.BlockSpec(memory_space=pltpu.VMEM),) * 3,
        scratch_shapes=[
            pltpu.VMEM((PIECES, 8, 16, *tile), f32),
            pltpu.VMEM((PIECES, 8, 16, *tile), f32),
            pltpu.VMEM((PIECES, 16, 8, *tile), f32),
            pltpu.VMEM((PIECES, 4, 4, 5, *tile), f32),
            pltpu.VMEM((PIECES, 3, 4, 5, *tile), f32),
            pltpu.VMEM((PIECES, 4, 5, *tile), f32),
            pltpu.VMEM((PIECES, 3, 5, *tile), f32),
            pltpu.SemaphoreType.DMA((PIECES,)),
            pltpu.SemaphoreType.DMA((PIECES,)),
            pltpu.SemaphoreType.DMA((PIECES,)),
            pltpu.SemaphoreType.DMA((PIECES,)),
            pltpu.SemaphoreType.DMA((PIECES,)),
            pltpu.SemaphoreType.DMA((4,)),
            pltpu.SemaphoreType.REGULAR((25,)),
            pltpu.SemaphoreType.REGULAR,
        ],
        compiler_params=pltpu.CompilerParams(collective_id=0, has_side_effects=True),
    )(tiles(pixel_stack), tiles(quality_weight))
    return pl.pallas_call(
        store,
        out_shape=tuple(jax.ShapeDtypeStruct(field.shape, field.dtype) for field in fitted),
        in_specs=[pl.BlockSpec(memory_space=pltpu.VMEM)] * 3,
        out_specs=(pl.BlockSpec(memory_space=pl.ANY),) * 3,
        scratch_shapes=[pltpu.SemaphoreType.DMA((2 + PARTS,))],
    )(*(pltpu.with_memory_space_constraint(field, pltpu.VMEM) for field in fitted))


def solution(mesh):
    return jax.shard_map(
        body,
        mesh=mesh,
        in_specs=(P(("wide", "narrow"), None, None), P(("wide", "narrow"), None, None)),
        out_specs=(P("wide", "narrow"), P("wide", "narrow"), P(None, "wide", "narrow")),
        check_vma=False,
    )
```
